128 devices in a mesh: pix: 32 (over x_lo, z, y), rep: 4 (over x_hi, core).
Axes of the slice: x: 4 (x_hi: 2, x_lo: 2; x = x_hi * 2 + x_lo), y: 4, z: 4, core: 2. Of those that a mesh axis runs over, the one named last changes fastest.
Arguments:
- interferograms: float32 [256, 524288], P(('pix', 'rep')), may hold values from -6 to 6
- epoch_pairs: int32 [2, 256], replicated, may hold values from 0 to 63, as said below
- los: float32 [3, 524288], P(None, ('pix', 'rep')), may hold values from 0.3 to 1
- patch_place: int32 [2, 4096], replicated, may hold values from 0 to 255, as said below
- patch_depth: int32 [4096], replicated, may hold values from 0 to 7
Outputs:
- predicted: float32 [64, 524288], P(None, ('pix', 'rep'))
- slip: float32 [64, 4096], P(None, ('pix', 'rep'))
The draws below stay inside these ranges and needn't reach their ends.
Inputs may be any that keep to these rules, and one draw needn't show every extreme that they name: `epoch_pairs`: row 0 holds an interferogram's earlier epoch and row 1 its later one; the two always differ. `patch_place`: row 0 is an east cell below 256; row 1 is a north cell below 128.
All inputs are finite; a program needn't handle non-finite values.
Results may differ from the reference program's by a relative error of at most 0.0037.
Values may be sent and summed in bfloat16 or wider, within the bound.
A program may use at most 64 MiB of HBM per device.

```python
import jax
import jax.numpy as jnp
from jax import lax

NEP = 64
NIFG = 256
NPATCH = 4096
IMG_W = 1024
SWEEPS = 2
PIX_DEV = 4096
NPIX = 524288
DEVICES = 128


def draw_epoch_pairs(key, part):
    first_key = jax.random.fold_in(key, 11)
    span_key = jax.random.fold_in(key, 12)
    primary = jax.random.randint(first_key, (NIFG,), 0, NEP - 1)
    spread = jax.random.randint(span_key, (NIFG,), 0, 1 << 20)
    secondary = primary + 1 + spread % (NEP - 1 - primary)
    return jnp.stack([primary, secondary]).astype(jnp.int32)


def draw_patch_place(key, part):
    north_cells = max(NPIX // (4 * IMG_W), 1)
    east = jax.random.randint(jax.random.fold_in(key, 31), (NPATCH,), 0, 256)
    north = jax.random.randint(jax.random.fold_in(key, 32), (NPATCH,), 0, north_cells)
    return jnp.stack([east, north]).astype(jnp.int32)


def draw_los(key, part):
    return jax.random.uniform(jax.random.fold_in(key, 41), (3, NPIX), jnp.float32, 0.3, 1.0)


def touch_ends(result, rng, least, high):
    shape = result.shape
    spot = [jax.random.randint(jax.random.fold_in(rng, axis), (), 0, shape[axis]) for axis in range(len(shape))]
    result = result.at[tuple(spot)].set(least)
    longest = shape.index(max(shape))
    spot[longest] = (spot[longest] + 1) % shape[longest]
    return result.at[tuple(spot)].set(high)


def level_of(rng, dims, split, least, high):
    level = 1.0
    for position, parts in split:
        draws = jax.random.uniform(jax.random.fold_in(jax.random.fold_in(rng, 6), position), (parts,), jnp.float32, least / len(split), high / len(split))
        level = level * jnp.repeat(jnp.exp(draws), dims[position] // parts).reshape((-1,) + (1,) * (len(dims) - 1 - position))
    return level


def centred(stream_key, shape, width, limit, cuts=(), kind=jnp.bfloat16):
    level = level_of(stream_key, shape, cuts, -0.22, 0.18) if cuts else 1.0
    values = jax.random.normal(stream_key, shape, jnp.float32) * width * level
    return jnp.minimum(jnp.maximum(values, -limit), limit).astype(kind)


def setup_inputs(seed: int = 0) -> dict:
    streams_of = jax.random.split(jax.random.key(seed), 6)
    return {
        "interferograms": centred(streams_of[0], (NIFG, NPIX), 1.0, 6.0, ((0, 128),), jnp.float32),
        "epoch_pairs": draw_epoch_pairs(jax.random.fold_in(streams_of[5], 71), 0),
        "los": draw_los(jax.random.fold_in(streams_of[5], 71), 0),
        "patch_place": draw_patch_place(jax.random.fold_in(streams_of[5], 71), 0),
        "patch_depth": touch_ends(jax.random.randint(streams_of[4], (NPATCH,), 0, 8), jax.random.fold_in(streams_of[4], 1), 0, 7).astype(jnp.int32),
    }


pixel_step = 0.1
patch_step = 0.4
damping = 0.5
depth_base = 0.5
depth_step = 0.25

def sbas_inverse(epoch_pairs):
    epochs = lax.iota(jnp.int32, NEP)
    design = (epochs[None, :] == epoch_pairs[1][:, None]).astype(jnp.float32) - (epochs[None, :] == epoch_pairs[0][:, None]).astype(jnp.float32)
    normal = jnp.dot(design.T, design, precision=lax.Precision.HIGHEST) + damping * jnp.eye(NEP, dtype=jnp.float32)
    factor = jnp.linalg.cholesky(normal)
    return jax.scipy.linalg.cho_solve((factor, True), design.T)

def green_tile(pixel, los_rows, patch_place, patch_depth):
    column = (pixel % IMG_W).astype(jnp.float32)
    line = (pixel // IMG_W).astype(jnp.float32)
    xpos = (column + 0.5) * pixel_step
    ypos = (line + 0.5) * pixel_step
    patch_x = (patch_place[0].astype(jnp.float32) + 0.5) * patch_step
    patch_y = (patch_place[1].astype(jnp.float32) + 0.5) * patch_step
    patch_z = depth_base + depth_step * patch_depth.astype(jnp.float32)
    delta_x = xpos[:, None] - patch_x[None, :]
    delta_y = ypos[:, None] - patch_y[None, :]
    delta_z = patch_z[None, :]
    dist_sq = delta_x * delta_x + delta_y * delta_y + delta_z * delta_z
    toward = los_rows[0][:, None] * delta_x + los_rows[1][:, None] * delta_y + los_rows[2][:, None] * delta_z
    return (delta_z * toward / (dist_sq * jnp.sqrt(dist_sq))).astype(jnp.bfloat16)

def reference(interferograms, epoch_pairs, los, patch_place, patch_depth):
    pseudo = sbas_inverse(epoch_pairs)
    series = jnp.dot(pseudo.astype(jnp.float32), interferograms.astype(jnp.float32), precision=lax.Precision.HIGHEST, preferred_element_type=jnp.float32)
    total = PIX_DEV * DEVICES
    blocks = total // PIX_DEV
    indices = jnp.arange(blocks, dtype=jnp.int32)

    def tile_at(index):
        start = index * PIX_DEV
        pixel = start + lax.iota(jnp.int32, PIX_DEV)
        los_rows = lax.dynamic_slice_in_dim(los, start, PIX_DEV, 1)
        return (green_tile(pixel, los_rows, patch_place, patch_depth), start)

    def first_step(carry, index):
        rhs, bound = carry
        tile, start = tile_at(index)
        resid = lax.dynamic_slice_in_dim(series, start, PIX_DEV, 1).astype(jnp.bfloat16)
        rhs = rhs + jnp.dot(resid.astype(jnp.float32), tile.astype(jnp.float32), preferred_element_type=jnp.float32)
        magnitude = jnp.abs(tile)
        weight = lax.optimization_barrier(jnp.sum(magnitude.astype(jnp.float32), axis=1)).astype(jnp.bfloat16)
        bound = bound + jnp.dot(weight[None, :].astype(jnp.float32), magnitude.astype(jnp.float32), preferred_element_type=jnp.float32)[0]
        return ((rhs, bound), None)
    zero_rhs = jnp.zeros((NEP, NPATCH), jnp.float32)
    zero_bound = jnp.zeros((NPATCH,), jnp.float32)
    (rhs, bound), unused = lax.scan(first_step, (zero_rhs, zero_bound), indices)
    slip = jnp.zeros((NEP, NPATCH), jnp.float32) + rhs / bound[None, :]
    for sweep in range(1, SWEEPS):
        slip_half = slip.astype(jnp.bfloat16)

        def sweep_step(rhs_now, index):
            tile, start = tile_at(index)
            guess = lax.dot_general(slip_half.astype(jnp.float32), tile.astype(jnp.float32), (((1,), (1,)), ((), ())), preferred_element_type=jnp.float32)
            resid = (lax.dynamic_slice_in_dim(series, start, PIX_DEV, 1) - guess).astype(jnp.bfloat16)
            return (rhs_now + jnp.dot(resid.astype(jnp.float32), tile.astype(jnp.float32), preferred_element_type=jnp.float32), None)
        rhs, unused = lax.scan(sweep_step, zero_rhs, indices)
        slip = slip + rhs / bound[None, :]
    slip_half = slip.astype(jnp.bfloat16)

    def final_block(index):
        tile, start = tile_at(index)
        return lax.dot_general(slip_half.astype(jnp.float32), tile.astype(jnp.float32), (((1,), (1,)), ((), ())), preferred_element_type=jnp.float32)
    pieces = lax.map(final_block, indices)
    predicted = jnp.transpose(pieces, (1, 0, 2)).reshape(NEP, total)
    return (predicted, slip)
```

```python
import jax
import jax.numpy as jnp
from jax import lax
from jax.experimental import pallas as pl
from jax.experimental.pallas import tpu as pltpu
from jax.sharding import PartitionSpec as P

NEP = 64
NPATCH = 4096
PIX_DEV = 4096
IMG_W = 1024
PIX = 32
REP = 4
DEV = PIX * REP
F32, BF = jnp.float32, jnp.bfloat16
MESH = pl.DeviceIdType.MESH
damping = 0.5


def split(x, n):
    out = []
    for _ in range(n):
        h = x.astype(BF).astype(F32)
        out.append(h)
        x = x - h
    return out


CB, PB = 64, 512


def green_kernel(los_ref, place_ref, depth_ref, g_ref, bound_ref, pixrow, pixcol, patchrow, patchf, prow, srow, wacc, wrow):
    base = (lax.axis_index("pix") * REP + lax.axis_index("rep")).astype(F32)
    cx = place_ref[0:1, :].astype(F32)
    ny = place_ref[1:2, :].astype(F32)
    d2 = depth_ref[...].astype(F32) + 2.0
    px = cx * 8.0 + 4.0
    py = (ny - base) * 8.0 + 3.0
    h = d2 * 5.0
    prow[0:1, :] = px
    for r in range(4):
        dy = 2.0 * r - py
        srow[r : r + 1, :] = dy * dy + h * h
    f1 = split(d2 * (px - 1024.0), 2)
    f2 = split(d2 * py, 2)
    rows = [d2] * 3 + [-f1[0], -f1[1]] * 3 + [-f2[0], -f2[1]] * 3 + [d2 * h] * 3
    patchrow[...] = jnp.zeros_like(patchrow)
    for k, v in enumerate(rows):
        patchrow[k : k + 1, :] = v
    patchf[...] = patchrow[...].astype(BF)
    g = lax.broadcasted_iota(jnp.int32, (1, PIX_DEV), 1)
    xc = ((g % IMG_W) * 2 + (1 - 1024)).astype(F32)
    yc = ((g // IMG_W) * 2).astype(F32)
    l0 = los_ref[0:1, :] * 100.0
    l1 = los_ref[1:2, :] * 100.0
    l2 = los_ref[2:3, :] * 100.0
    a = split(l0 * xc + l1 * yc, 3)
    s0, s1, s2 = split(l0, 3), split(l1, 3), split(l2, 3)
    rows = a + [s0[0], s0[0], s0[1], s0[1], s0[2], s0[2]] + [s1[0], s1[0], s1[1], s1[1], s1[2], s1[2]] + s2
    pixrow[...] = jnp.zeros_like(pixrow)
    for k, v in enumerate(rows):
        pixrow[k : k + 1, :] = v
    pixcol[...] = pixrow[...].T.astype(BF)
    wacc[...] = jnp.zeros_like(wacc)

    def step(it, _):
        c0 = pl.multiple_of((it // (NPATCH // PB)) * CB, CB)
        p0 = pl.multiple_of((it % (NPATCH // PB)) * PB, PB)
        xs = (lax.broadcasted_iota(jnp.int32, (CB, 128), 0) * 2 + (2 * c0 + 1)).astype(F32)
        for r in range(4):
            rowsl = pl.ds(pl.multiple_of(r * IMG_W + c0, CB), CB)
            t = jnp.dot(pixcol[rowsl, :], patchf[:, pl.ds(p0, PB)], preferred_element_type=F32)
            acc = wacc[rowsl, :]
            for q in range(PB // 128):
                ps = pl.ds(pl.multiple_of(p0 + 128 * q, 128), 128)
                dx = xs - prow[0:1, ps]
                r2 = dx * dx + srow[r : r + 1, ps]
                inv = lax.rsqrt(r2)
                gf = t[:, 128 * q : 128 * q + 128] * (inv * inv * inv)
                acc = acc + jnp.abs(gf)
                g_ref[rowsl, ps] = gf.astype(BF)
            wacc[rowsl, :] = acc
        return 0

    lax.fori_loop(0, (IMG_W // CB) * (NPATCH // PB), step, 0)

    ones = jnp.ones((16, 128), BF)

    def wstep(j, _):
        sl = pl.ds(pl.multiple_of(j * 512, 512), 512)
        w = jnp.zeros((16, 512), F32)
        for part in split(wacc[sl, :], 3):
            w = w + lax.dot_general(ones, part.astype(BF), (((1,), (1,)), ((), ())), preferred_element_type=F32)
        wrow[:, sl] = w.astype(BF)
        return 0

    lax.fori_loop(0, 8, wstep, 0)

    def bstep(j, _):
        ps = pl.ds(pl.multiple_of(j * 256, 256), 256)
        b = jnp.dot(wrow[...], jnp.abs(g_ref[:, ps]), preferred_element_type=F32)
        bound_ref[2 * j] = b[0:1, 0:128]
        bound_ref[2 * j + 1] = b[0:1, 128:256]
        return 0

    lax.fori_loop(0, 16, bstep, 0)


def green(los, place, depth):
    vm = pl.BlockSpec(memory_space=pltpu.VMEM)
    return pl.pallas_call(
        green_kernel,
        out_shape=(pltpu.VMEM((PIX_DEV, NPATCH), BF), jax.ShapeDtypeStruct((PIX, 1, 128), F32)),
        in_specs=[vm] * 3,
        out_specs=(vm, vm),
        scratch_shapes=[
            pltpu.VMEM((24, PIX_DEV), F32),
            pltpu.VMEM((PIX_DEV, 24), BF),
            pltpu.VMEM((24, NPATCH), F32),
            pltpu.VMEM((24, NPATCH), BF),
            pltpu.VMEM((8, NPATCH), F32),
            pltpu.VMEM((8, NPATCH), F32),
            pltpu.VMEM((PIX_DEV, 128), F32),
            pltpu.VMEM((16, PIX_DEV), BF),
        ],
        compiler_params=pltpu.CompilerParams(vmem_limit_bytes=16 << 20),
        cost_estimate=pl.CostEstimate(flops=30_000_000_000, bytes_accessed=1 << 20, transcendentals=0),
        name="green",
    )(los, place, depth)


CH = (16, 128)


def sweeps_kernel(
    g_ref, series_ref, bound_ref, pred_ref, slip_ref,
    resid, send1, send2, recv1, recv2, brecv, own, all1, all2, slipf,
    ssem, rsem,
):
    mp, mr = lax.axis_index("pix"), lax.axis_index("rep")
    me = mp * REP + mr

    def to(dst):
        return {"pix": dst // REP, "rep": dst % REP}

    def copy(src, dst, k, dev):
        return pltpu.make_async_remote_copy(src, dst, ssem.at[k], rsem.at[k], device_id=to(dev), device_id_type=MESH)

    def wait_sent(buf, k):
        pltpu.make_async_copy(buf, buf, ssem.at[k]).wait()

    def wait_got(buf, k):
        pltpu.make_async_copy(buf, buf, rsem.at[k]).wait()

    def bound_send(k, _):
        dst = lax.rem(me + k, DEV)
        copy(bound_ref.at[dst // REP], brecv.at[DEV - k], 0, dst).start()
        return 0

    lax.fori_loop(1, DEV, bound_send, 0)
    brecv[0] = bound_ref[mp]

    def project(send, recv, k):
        def push(j):
            pc = lax.rem(mp // 2 + j, 16)
            for q in range(2):
                for eb in range(REP):
                    dst = (2 * pc + q) * REP + eb

                    @pl.when(dst != me)
                    def _():
                        copy(send.at[2 * pc + q, eb], recv.at[lax.rem(me - dst + DEV, DEV)], k, dst).start()

        def step(j, _):
            pc = lax.rem(mp // 2 + j, 16)
            rhs = jnp.dot(resid[...], g_ref[:, pl.ds(pl.multiple_of(pc * 256, 256), 256)], preferred_element_type=F32)
            for q in range(2):
                for eb in range(REP):
                    send[2 * pc + q, eb] = rhs[16 * eb : 16 * eb + 16, 128 * q : 128 * q + 128].astype(BF)

            @pl.when(j > 0)
            def _():
                push(j - 1)

            return 0

        lax.fori_loop(0, 16, step, 0)
        push(15)
        recv[0] = send[mp, mr]
        wait_got(recv.at[pl.ds(1, DEV - 1)], k)

        def add(i, acc):
            return acc + recv[i].astype(F32)

        return lax.fori_loop(0, DEV, add, jnp.zeros(CH, F32))

    def share(buf, k):
        def one(i, _):
            copy(own.at[k], buf.at[mp, mr], 1 + k, lax.rem(me + i, DEV)).start()
            return 0

        lax.fori_loop(1, DEV, one, 0)
        buf[mp, mr] = own[k]
        wait_got(recv1.at[pl.ds(1, DEV - 1)], 1 + k)

    def flat(buf):
        return jnp.concatenate([buf[b].reshape(NEP, 128) for b in range(PIX)], axis=1)

    resid[...] = series_ref[...].astype(BF)
    rhs = project(send1, recv1, 3)
    wait_got(brecv.at[pl.ds(1, DEV - 1)], 0)

    def badd(i, acc):
        return acc + brecv[i]

    bound = lax.fori_loop(0, DEV, badd, jnp.zeros((1, 128), F32))
    slip = rhs / bound
    own[0] = slip.astype(BF)
    share(all1, 0)
    slipf[...] = flat(all1)

    def guess(j, _):
        gs = pl.ds(pl.multiple_of(j * 256, 256), 256)
        out = lax.dot_general(slipf[...], g_ref[gs, :], (((1,), (1,)), ((), ())), preferred_element_type=F32)
        resid[:, gs] = (series_ref[:, gs] - out).astype(BF)
        return 0

    lax.fori_loop(0, 16, guess, 0)
    rhs = project(send2, recv2, 4)
    slip = slip + rhs / bound
    own[1] = slip.astype(BF)
    share(all2, 1)
    slipf[...] = flat(all2)

    def final(j, _):
        gs = pl.ds(pl.multiple_of(j * 256, 256), 256)
        pred_ref[:, gs] = lax.dot_general(slipf[...], g_ref[gs, :], (((1,), (1,)), ((), ())), preferred_element_type=F32)
        return 0

    lax.fori_loop(0, 16, final, 0)
    block = all2[mp].reshape(NEP, 128).astype(F32)
    slip_ref[...] = pltpu.roll(block, lax.rem(128 - 32 * mr, 128), 1)
    wait_sent(brecv.at[pl.ds(1, DEV - 1)], 0)
    for k in range(1, 5):
        wait_sent(recv1.at[pl.ds(1, DEV - 1)], k)


def sweeps(g, series, bound):
    vm = pl.BlockSpec(memory_space=pltpu.VMEM)
    return pl.pallas_call(
        sweeps_kernel,
        out_shape=(jax.ShapeDtypeStruct((NEP, PIX_DEV), F32), jax.ShapeDtypeStruct((NEP, 128), F32)),
        in_specs=[vm] * 3,
        out_specs=(vm, vm),
        scratch_shapes=[
            pltpu.VMEM((NEP, PIX_DEV), BF),
            pltpu.VMEM((PIX, REP) + CH, BF),
            pltpu.VMEM((PIX, REP) + CH, BF),
            pltpu.VMEM((DEV,) + CH, BF),
            pltpu.VMEM((DEV,) + CH, BF),
            pltpu.VMEM((DEV, 1, 128), F32),
            pltpu.VMEM((2,) + CH, BF),
            pltpu.VMEM((PIX, REP) + CH, BF),
            pltpu.VMEM((PIX, REP) + CH, BF),
            pltpu.VMEM((NEP, NPATCH), BF),
            pltpu.SemaphoreType.DMA((5,)),
            pltpu.SemaphoreType.DMA((5,)),
        ],
        compiler_params=pltpu.CompilerParams(vmem_limit_bytes=44 << 20, has_side_effects=True),
        name="sweeps",
    )(g, series, bound)


def sbas_inverse(epoch_pairs):
    epochs = lax.iota(jnp.int32, NEP)
    design = (epochs[None, :] == epoch_pairs[1][:, None]).astype(F32) - (epochs[None, :] == epoch_pairs[0][:, None]).astype(F32)
    normal = jnp.dot(design.T, design, precision=lax.Precision.HIGHEST) + damping * jnp.eye(NEP, dtype=F32)
    factor = jnp.linalg.cholesky(normal)
    return jax.scipy.linalg.cho_solve((factor, True), design.T)


def on_device(interferograms, epoch_pairs, los, patch_place, patch_depth):
    ifg_dev = interferograms.shape[0]
    pieces = interferograms.astype(BF).reshape(ifg_dev, DEV, PIX_DEV)
    got = lax.all_to_all(pieces, ("pix", "rep"), split_axis=1, concat_axis=0, tiled=True)[:, 0, :]
    g, bound = green(los, patch_place, patch_depth.reshape(1, NPATCH))
    pseudo = sbas_inverse(epoch_pairs)
    high = lax.reduce_precision(pseudo, 8, 7)
    parts = jnp.concatenate([high, pseudo - high]).astype(BF)
    both = jnp.dot(parts, got, preferred_element_type=F32)
    series = both[:NEP] + both[NEP:]
    predicted, slip = sweeps(g, series, bound)
    return predicted, slip[:, :32]


def solution(mesh):
    placed = (P(("pix", "rep"), None), P(), P(None, ("pix", "rep")), P(), P())
    return jax.shard_map(
        on_device,
        mesh=mesh,
        in_specs=placed,
        out_specs=(P(None, ("pix", "rep")), P(None, ("pix", "rep"))),
        check_vma=False,
    )
```

```python
import jax
import jax.numpy as jnp
from jax import lax
from jax.experimental import pallas as pl
from jax.experimental.pallas import tpu as pltpu
from jax.sharding import PartitionSpec as P

NEP = 64
NPATCH = 4096
PIX_DEV = 4096
IMG_W = 1024
PIX = 32
REP = 4
DEV = PIX * REP
F32, BF = jnp.float32, jnp.bfloat16
MESH = pl.DeviceIdType.MESH
damping = 0.5


def split(x, n):
    out = []
    for _ in range(n):
        h = x.astype(BF).astype(F32)
        out.append(h)
        x = x - h
    return out

CB, PB = 64, 512
NCHUNK = 512
CH = (16, 128)


def features(los_ref, place_ref, depth_ref, pixrow, pixcol, patchrow, patchf, prow, srow):
    base = (lax.axis_index("pix") * REP + lax.axis_index("rep")).astype(F32)
    cx = place_ref[0:1, :].astype(F32)
    ny = place_ref[1:2, :].astype(F32)
    d2 = depth_ref[...].astype(F32) + 2.0
    px = cx * 8.0 + 4.0
    py = (ny - base) * 8.0 + 3.0
    h = d2 * 5.0
    prow[0:1, :] = px
    for r in range(4):
        dy = 2.0 * r - py
        srow[r : r + 1, :] = dy * dy + h * h
    f1 = split(d2 * (px - 1024.0), 2)
    f2 = split(d2 * py, 2)
    rows = [d2] * 3 + [-f1[0], -f1[1]] * 3 + [-f2[0], -f2[1]] * 3 + [d2 * h] * 3
    patchrow[...] = jnp.zeros_like(patchrow)
    for k, v in enumerate(rows):
        patchrow[k : k + 1, :] = v
    patchf[...] = patchrow[...].astype(BF)
    g = lax.broadcasted_iota(jnp.int32, (1, PIX_DEV), 1)
    xc = ((g % IMG_W) * 2 + (1 - 1024)).astype(F32)
    yc = ((g // IMG_W) * 2).astype(F32)
    l0 = los_ref[0:1, :] * 100.0
    l1 = los_ref[1:2, :] * 100.0
    l2 = los_ref[2:3, :] * 100.0
    a = split(l0 * xc + l1 * yc, 3)
    s0, s1, s2 = split(l0, 3), split(l1, 3), split(l2, 3)
    rows = a + [s0[0], s0[0], s0[1], s0[1], s0[2], s0[2]] + [s1[0], s1[0], s1[1], s1[1], s1[2], s1[2]] + s2
    pixrow[...] = jnp.zeros_like(pixrow)
    for k, v in enumerate(rows):
        pixrow[k : k + 1, :] = v
    pixcol[...] = pixrow[...].T.astype(BF)


def invert_step(k, a_ref):
    a = a_ref[...]
    kk = lax.rem(k, NEP)
    lane = lax.broadcasted_iota(jnp.int32, (NEP, NEP), 1)
    sub = lax.broadcasted_iota(jnp.int32, (NEP, NEP), 0)
    row = a_ref[pl.ds(kk, 1), :]
    lane1 = lax.broadcasted_iota(jnp.int32, (1, NEP), 1)
    inv = 1.0 / jnp.sum(jnp.where(lane1 == kk, row, 0.0), axis=1, keepdims=True)
    col = jnp.sum(jnp.where(lane == kk, a, 0.0), axis=1, keepdims=True)
    new_row = jnp.where(lane1 == kk, inv, row * inv)
    rest = jnp.where(lane == kk, 0.0, a) - col * new_row
    new = jnp.where(sub == kk, new_row, rest)
    a_ref[...] = jnp.where(k < NEP, new, a)


def kernel(
    x_ref, pairs_ref, los_ref, place_ref, depth_ref, pred_ref, slip_ref,
    g_ref, pixrow, pixcol, patchrow, patchf, prow, srow, wacc, wrow, a_ref, bound_ref,
    got, series, resid, send1, send2, recv1, recv2, brecv, own, all1, all2, slipf, blk,
    ssem, rsem, lsem,
):
    mp, mr = lax.axis_index("pix"), lax.axis_index("rep")
    me = mp * REP + mr

    def to(dst):
        return {"pix": dst // REP, "rep": lax.rem(dst, REP)}

    def copy(src, dst, k, dev):
        return pltpu.make_async_remote_copy(src, dst, ssem.at[k], rsem.at[k], device_id=to(dev), device_id_type=MESH)

    def wait_sent(buf, k):
        pltpu.make_async_copy(buf, buf, ssem.at[k]).wait()

    def wait_got(buf, k):
        pltpu.make_async_copy(buf, buf, rsem.at[k]).wait()

    def others(fn):
        def one(k, _):
            fn(k, lax.rem(me + k, DEV))
            return 0

        lax.fori_loop(1, DEV, one, 0)

    others(lambda k, dst: copy(x_ref.at[dst], got.at[me], 0, dst).start())
    mine = pltpu.make_async_copy(x_ref.at[me], got.at[me], lsem)
    mine.start()

    features(los_ref, place_ref, depth_ref, pixrow, pixcol, patchrow, patchf, prow, srow)
    epoch = lax.broadcasted_iota(jnp.int32, (NEP, 256), 0)
    design_t = (epoch == pairs_ref[1:2, :]).astype(F32) - (epoch == pairs_ref[0:1, :]).astype(F32)
    design_b = design_t.astype(BF)
    normal = lax.dot_general(design_b, design_b, (((1,), (1,)), ((), ())), preferred_element_type=F32)
    eye = lax.broadcasted_iota(jnp.int32, (NEP, NEP), 0) == lax.broadcasted_iota(jnp.int32, (NEP, NEP), 1)
    a_ref[...] = normal + jnp.where(eye, damping, 0.0)
    wacc[...] = jnp.zeros_like(wacc)

    def step(it, _):
        invert_step(it, a_ref)
        c0 = pl.multiple_of((it // (NPATCH // PB)) * CB, CB)
        p0 = pl.multiple_of(lax.rem(it, NPATCH // PB) * PB, PB)
        xs = (lax.broadcasted_iota(jnp.int32, (CB, 128), 0) * 2 + (2 * c0 + 1)).astype(F32)
        dxs = []
        for q in range(PB // 128):
            dx = xs - prow[0:1, pl.ds(pl.multiple_of(p0 + 128 * q, 128), 128)]
            dxs.append(dx * dx)
        for r in range(4):
            rowsl = pl.ds(pl.multiple_of(r * IMG_W + c0, CB), CB)
            t = jnp.dot(pixcol[rowsl, :], patchf[:, pl.ds(p0, PB)], preferred_element_type=F32)
            acc = wacc[rowsl, :]
            for q in range(PB // 128):
                ps = pl.ds(pl.multiple_of(p0 + 128 * q, 128), 128)
                inv = lax.rsqrt(dxs[q] + srow[r : r + 1, ps])
                gf = t[:, 128 * q : 128 * q + 128] * (inv * inv * inv)
                acc = acc + jnp.abs(gf)
                g_ref[rowsl, ps] = gf.astype(BF)
            wacc[rowsl, :] = acc
        return 0

    lax.fori_loop(0, (IMG_W // CB) * (NPATCH // PB), step, 0)

    ones = jnp.ones((16, 128), BF)

    def wstep(j, _):
        sl = pl.ds(pl.multiple_of(j * 512, 512), 512)
        w = jnp.zeros((16, 512), F32)
        for part in split(wacc[sl, :], 3):
            w = w + lax.dot_general(ones, part.astype(BF), (((1,), (1,)), ((), ())), preferred_element_type=F32)
        wrow[:, sl] = w.astype(BF)
        return 0

    lax.fori_loop(0, 8, wstep, 0)

    def bstep(j, _):
        ps = pl.ds(pl.multiple_of(j * NCHUNK, NCHUNK), NCHUNK)
        b = jnp.dot(wrow[...], jnp.abs(g_ref[:, ps]), preferred_element_type=F32)
        for q in range(NCHUNK // 128):
            bound_ref[j * (NCHUNK // 128) + q] = b[0:1, 128 * q : 128 * q + 128]
        return 0

    lax.fori_loop(0, NPATCH // NCHUNK, bstep, 0)

    others(lambda k, dst: copy(bound_ref.at[dst // REP], brecv.at[DEV - k], 1, dst).start())
    brecv[0] = bound_ref[mp]

    acc = jnp.zeros((NEP, 256), F32)
    for part in split(a_ref[...], 3):
        acc = acc + jnp.dot(part.astype(BF), design_b, preferred_element_type=F32)
    parts = split(acc, 2)
    pseudo = jnp.concatenate(parts, axis=0).astype(BF)
    mine.wait()
    wait_got(got.at[pl.ds(1, DEV - 1)], 0)

    def sstep(k, _):
        sl = pl.ds(pl.multiple_of(k * 256, 256), 256)
        out = jnp.dot(pseudo, got[:, :, sl].reshape(256, 256), preferred_element_type=F32)
        ser = out[:NEP] + out[NEP:]
        series[:, sl] = ser
        high, low = split(ser, 2)
        resid[0:NEP, sl] = high.astype(BF)
        resid[NEP : 2 * NEP, sl] = low.astype(BF)
        return 0

    lax.fori_loop(0, 16, sstep, 0)

    per = NCHUNK // 128

    def project(send, recv, k):
        def push(j):
            pc = lax.rem(mp // per + j, PIX // per)

            def one(i, _):
                dst = pc * (per * REP) + i

                @pl.when(dst != me)
                def _():
                    copy(send.at[dst // REP, lax.rem(dst, REP)], recv.at[lax.rem(me - dst + DEV, DEV)], k, dst).start()

                return 0

            lax.fori_loop(0, per * REP, one, 0)

        def step(j, _):
            pc = lax.rem(mp // per + j, PIX // per)
            out = jnp.dot(resid[...], g_ref[:, pl.ds(pl.multiple_of(pc * NCHUNK, NCHUNK), NCHUNK)], preferred_element_type=F32)
            rhs = (out[:NEP] + out[NEP:]).astype(BF)
            for q in range(per):
                for eb in range(REP):
                    send[per * pc + q, eb] = rhs[16 * eb : 16 * eb + 16, 128 * q : 128 * q + 128]

            @pl.when(j > 0)
            def _():
                push(j - 1)

            return 0

        lax.fori_loop(0, PIX // per, step, 0)
        push(PIX // per - 1)
        recv[0] = send[mp, mr]
        wait_got(recv.at[pl.ds(1, DEV - 1)], k)
        return jnp.sum(recv[...].astype(F32), axis=0)

    def share(buf, i, k):
        others(lambda n, dst: copy(own.at[i], buf.at[mp, mr], k, dst).start())
        buf[mp, mr] = own[i]
        wait_got(recv1.at[pl.ds(1, DEV - 1)], k)
        for b in range(PIX):
            slipf[:, 128 * b : 128 * b + 128] = buf[b].reshape(NEP, 128)

    rhs = project(send1, recv1, 2)
    wait_got(brecv.at[pl.ds(1, DEV - 1)], 1)
    bound = jnp.sum(brecv[...], axis=0)
    slip = rhs / bound
    own[0] = slip.astype(BF)
    share(all1, 0, 3)

    def guess(j, _):
        gs = pl.ds(pl.multiple_of(j * NCHUNK, NCHUNK), NCHUNK)
        out = lax.dot_general(slipf[...], g_ref[gs, :], (((1,), (1,)), ((), ())), preferred_element_type=F32)
        high, low = split(series[:, gs] - out, 2)
        resid[0:NEP, gs] = high.astype(BF)
        resid[NEP : 2 * NEP, gs] = low.astype(BF)
        return 0

    lax.fori_loop(0, PIX_DEV // NCHUNK, guess, 0)
    rhs = project(send2, recv2, 4)
    slip = slip + rhs / bound
    own[1] = slip.astype(BF)
    blk[mr] = slip
    for i in range(1, REP):
        pltpu.make_async_remote_copy(
            blk.at[mr], blk.at[mr], ssem.at[6], rsem.at[6], device_id={"pix": mp, "rep": lax.rem(mr + i, REP)}, device_id_type=MESH
        ).start()
    share(all2, 1, 5)

    def final(j, _):
        gs = pl.ds(pl.multiple_of(j * NCHUNK, NCHUNK), NCHUNK)
        pred_ref[:, gs] = lax.dot_general(slipf[...], g_ref[gs, :], (((1,), (1,)), ((), ())), preferred_element_type=F32)
        return 0

    lax.fori_loop(0, PIX_DEV // NCHUNK, final, 0)
    wait_got(blk.at[pl.ds(1, REP - 1)], 6)
    slip_ref[...] = pltpu.roll(blk[...].reshape(NEP, 128), lax.rem(128 - 32 * mr, 128), 1)
    wait_sent(got.at[pl.ds(1, DEV - 1)], 0)
    wait_sent(brecv.at[pl.ds(1, DEV - 1)], 1)
    for k in range(2, 6):
        wait_sent(recv1.at[pl.ds(1, DEV - 1)], k)
    wait_sent(blk.at[pl.ds(1, REP - 1)], 6)


def on_device(interferograms, epoch_pairs, los, patch_place, patch_depth):
    x = interferograms.astype(BF).reshape(2, DEV, PIX_DEV).transpose(1, 0, 2)
    vm = pl.BlockSpec(memory_space=pltpu.VMEM)
    predicted, slip = pl.pallas_call(
        kernel,
        out_shape=(jax.ShapeDtypeStruct((NEP, PIX_DEV), F32), jax.ShapeDtypeStruct((NEP, 128), F32)),
        in_specs=[pl.BlockSpec(memory_space=pl.ANY)] + [vm] * 4,
        out_specs=(vm, vm),
        scratch_shapes=[
            pltpu.VMEM((PIX_DEV, NPATCH), BF),
            pltpu.VMEM((24, PIX_DEV), F32),
            pltpu.VMEM((PIX_DEV, 24), BF),
            pltpu.VMEM((24, NPATCH), F32),
            pltpu.VMEM((24, NPATCH), BF),
            pltpu.VMEM((8, NPATCH), F32),
            pltpu.VMEM((8, NPATCH), F32),
            pltpu.VMEM((PIX_DEV, 128), F32),
            pltpu.VMEM((16, PIX_DEV), BF),
            pltpu.VMEM((NEP, NEP), F32),
            pltpu.VMEM((PIX, 1, 128), F32),
            pltpu.VMEM((DEV, 2, PIX_DEV), BF),
            pltpu.VMEM((NEP, PIX_DEV), F32),
            pltpu.VMEM((2 * NEP, PIX_DEV), BF),
            pltpu.VMEM((PIX, REP) + CH, BF),
            pltpu.VMEM((PIX, REP) + CH, BF),
            pltpu.VMEM((DEV,) + CH, BF),
            pltpu.VMEM((DEV,) + CH, BF),
            pltpu.VMEM((DEV, 1, 128), F32),
            pltpu.VMEM((2,) + CH, BF),
            pltpu.VMEM((PIX, REP) + CH, BF),
            pltpu.VMEM((PIX, REP) + CH, BF),
            pltpu.VMEM((NEP, NPATCH), BF),
            pltpu.VMEM((REP,) + CH, F32),
            pltpu.SemaphoreType.DMA((7,)),
            pltpu.SemaphoreType.DMA((7,)),
            pltpu.SemaphoreType.DMA(()),
        ],
        compiler_params=pltpu.CompilerParams(vmem_limit_bytes=60 << 20, has_side_effects=True),
        name="slip",
    )(x, epoch_pairs, los, patch_place, patch_depth.reshape(1, NPATCH))
    return predicted, slip[:, :32]


def solution(mesh):
    placed = (P(("pix", "rep"), None), P(), P(None, ("pix", "rep")), P(), P())
    return jax.shard_map(
        on_device,
        mesh=mesh,
        in_specs=placed,
        out_specs=(P(None, ("pix", "rep")), P(None, ("pix", "rep"))),
        check_vma=False,
    )
```

```python
import functools

import jax
import jax.numpy as jnp
from jax import lax
from jax.experimental import pallas as pl
from jax.experimental.pallas import tpu as pltpu
from jax.sharding import PartitionSpec as P

NEP = 64
NPATCH = 4096
PIX_DEV = 4096
IMG_W = 1024
PIX = 32
REP = 4
DEV = PIX * REP
F32, BF = jnp.float32, jnp.bfloat16
MESH = pl.DeviceIdType.MESH
damping = 0.5


def split(x, n):
    out = []
    for _ in range(n):
        h = x.astype(BF).astype(F32)
        out.append(h)
        x = x - h
    return out

CB, PB = 64, 512
NCHUNK = 512
PEERS = DEV // 2
CH = (16, 128)


def features(los_ref, place_ref, depth_ref, pixrow, pixcol, patchrow, patchf, prow, srow):
    base = (lax.axis_index("pix") * REP + lax.axis_index("rep")).astype(F32)
    cx = place_ref[0:1, :].astype(F32)
    ny = place_ref[1:2, :].astype(F32)
    d2 = depth_ref[...].astype(F32) + 2.0
    px = cx * 8.0 + 4.0
    py = (ny - base) * 8.0 + 3.0
    h = d2 * 5.0
    prow[0:1, :] = px
    for r in range(4):
        dy = 2.0 * r - py
        srow[r : r + 1, :] = dy * dy + h * h
    f1 = split(d2 * (px - 1024.0), 2)
    f2 = split(d2 * py, 2)
    rows = [d2] * 3 + [-f1[0], -f1[1]] * 3 + [-f2[0], -f2[1]] * 3 + [d2 * h] * 3
    patchrow[...] = jnp.zeros_like(patchrow)
    for k, v in enumerate(rows):
        patchrow[k : k + 1, :] = v
    patchf[...] = patchrow[...].astype(BF)
    g = lax.broadcasted_iota(jnp.int32, (1, PIX_DEV), 1)
    xc = ((g % IMG_W) * 2 + (1 - 1024)).astype(F32)
    yc = ((g // IMG_W) * 2).astype(F32)
    l0 = los_ref[0:1, :] * 100.0
    l1 = los_ref[1:2, :] * 100.0
    l2 = los_ref[2:3, :] * 100.0
    a = split(l0 * xc + l1 * yc, 3)
    s0, s1, s2 = split(l0, 3), split(l1, 3), split(l2, 3)
    rows = a + [s0[0], s0[0], s0[1], s0[1], s0[2], s0[2]] + [s1[0], s1[0], s1[1], s1[1], s1[2], s1[2]] + s2
    pixrow[...] = jnp.zeros_like(pixrow)
    for k, v in enumerate(rows):
        pixrow[k : k + 1, :] = v
    pixcol[...] = pixrow[...].T.astype(BF)


def invert_step(k, a_ref):
    a = a_ref[...]
    kk = lax.rem(k, NEP)
    lane = lax.broadcasted_iota(jnp.int32, (NEP, NEP), 1)
    sub = lax.broadcasted_iota(jnp.int32, (NEP, NEP), 0)
    row = a_ref[pl.ds(kk, 1), :]
    lane1 = lax.broadcasted_iota(jnp.int32, (1, NEP), 1)
    inv = 1.0 / jnp.sum(jnp.where(lane1 == kk, row, 0.0), axis=1, keepdims=True)
    col = jnp.sum(jnp.where(lane == kk, a, 0.0), axis=1, keepdims=True)
    new_row = jnp.where(lane1 == kk, inv, row * inv)
    rest = jnp.where(lane == kk, 0.0, a) - col * new_row
    new = jnp.where(sub == kk, new_row, rest)
    a_ref[...] = jnp.where(k < NEP, new, a)


def kernel(*refs):
    pl.run_scoped(
        functools.partial(body, *refs),
        pltpu.VMEM((PIX_DEV, NPATCH), BF),
        pltpu.VMEM((PIX_DEV, 24), BF),
        pltpu.VMEM((24, NPATCH), BF),
        pltpu.VMEM((16, PIX_DEV), BF),
        pltpu.VMEM((2 * NEP, PIX_DEV), BF),
        pltpu.VMEM((NEP, NPATCH // 2), BF),
    )


def body(
    x_ref, pairs_ref, los_ref, place_ref, depth_ref, pred_ref, slip_ref,
    pixrow, patchrow, prow, srow, wacc, a_ref, bound_ref,
    got, series, send1, send2, recv1, recv2, psend1, psend2, precv1, precv2, bpair, bsend, brecv, own, all1, all2, fine, blk,
    ssem, rsem, lsem,
    g_ref, pixcol, patchf, wrow, resid, slipf,
):
    mp, mr = lax.axis_index("pix"), lax.axis_index("rep")
    me = mp * REP + mr

    def copy(src, dst, k, pix, rep):
        return pltpu.make_async_remote_copy(src, dst, ssem.at[k], rsem.at[k], device_id={"pix": pix, "rep": rep}, device_id_type=MESH)

    def wait_sent(buf, k):
        pltpu.make_async_copy(buf, buf, ssem.at[k]).wait()

    def wait_got(buf, k):
        pltpu.make_async_copy(buf, buf, rsem.at[k]).wait()

    def others(fn):
        for i in range(1, REP):
            fn(mp, lax.rem(mr + i, REP))

        def one(k, _):
            pix = lax.rem(mp + k, PIX)
            for rep in range(REP):
                fn(pix, rep)
            return 0

        lax.fori_loop(1, PIX, one, 0)

    ready = pltpu.get_barrier_semaphore()
    with jax.named_scope("signal"):
        others(lambda pix, rep: pl.semaphore_signal(ready, inc=1, device_id={"pix": pix, "rep": rep}, device_id_type=MESH))
    with jax.named_scope("features"):
        features(los_ref, place_ref, depth_ref, pixrow, pixcol, patchrow, patchf, prow, srow)
    with jax.named_scope("wait_ready"):
        pl.semaphore_wait(ready, DEV - 1)

    mc, mx = lax.rem(mr, 2), mr // 2
    mine_at = 2 * mp + mx
    pb_own, eb_own = 16 * mc + mp // 2, 2 * mx + lax.rem(mp, 2)

    def pair(src, dst, k):
        return copy(src, dst, k, mp, mr + 1 - 2 * mc)

    got_pair = wait_got

    def peers(fn):
        for i in range(1, 4):
            at = lax.rem(2 * lax.rem(mp, 2) + mx + i, 4)
            fn(mp // 2, at // 2, lax.rem(at, 2))

        def one(k, _):
            pp = lax.rem(mp // 2 + k, 16)
            for half in range(2):
                for xh in range(2):
                    fn(pp, half, xh)
            return 0

        lax.fori_loop(1, 16, one, 0)

    with jax.named_scope("send_ifg"):
        others(lambda pix, rep: copy(x_ref.at[pix * REP + rep], got.at[me], 0, pix, rep).start())
        mine = pltpu.make_async_copy(x_ref.at[me], got.at[me], lsem)
        mine.start()

    with jax.named_scope("normal"):
        epoch = lax.broadcasted_iota(jnp.int32, (NEP, 256), 0)
        design_t = (epoch == pairs_ref[1:2, :]).astype(F32) - (epoch == pairs_ref[0:1, :]).astype(F32)
        design_b = design_t.astype(BF)
        normal = lax.dot_general(design_b, design_b, (((1,), (1,)), ((), ())), preferred_element_type=F32)
        eye = lax.broadcasted_iota(jnp.int32, (NEP, NEP), 0) == lax.broadcasted_iota(jnp.int32, (NEP, NEP), 1)
        a_ref[...] = normal + jnp.where(eye, damping, 0.0)
        wacc[...] = jnp.zeros_like(wacc)

    def step(it, _):
        invert_step(it, a_ref)
        c0 = pl.multiple_of((it // (NPATCH // PB)) * CB, CB)
        p0 = pl.multiple_of(lax.rem(it, NPATCH // PB) * PB, PB)
        xs = (lax.broadcasted_iota(jnp.int32, (CB, 128), 0) * 2 + (2 * c0 + 1)).astype(F32)
        dxs = []
        for q in range(PB // 128):
            dx = xs - prow[0:1, pl.ds(pl.multiple_of(p0 + 128 * q, 128), 128)]
            dxs.append(dx * dx)
        for r in range(4):
            rowsl = pl.ds(pl.multiple_of(r * IMG_W + c0, CB), CB)
            t = jnp.dot(pixcol[rowsl, :], patchf[:, pl.ds(p0, PB)], preferred_element_type=F32)
            acc = wacc[rowsl, :]
            mags = []
            for q in range(PB // 128):
                ps = pl.ds(pl.multiple_of(p0 + 128 * q, 128), 128)
                inv = lax.rsqrt(dxs[q] + srow[r : r + 1, ps])
                gf = (t[:, 128 * q : 128 * q + 128] * (inv * inv * inv)).astype(BF)
                g_ref[rowsl, ps] = gf
                mags.append(jnp.abs(gf))
            while len(mags) > PB // 512:
                mags = [a + b for a, b in zip(mags[0::2], mags[1::2])]
            for m in mags:
                acc = acc + m.astype(F32)
            wacc[rowsl, :] = acc
        return 0

    with jax.named_scope("green"):
        lax.fori_loop(0, (IMG_W // CB) * (NPATCH // PB), step, 0)

    ones = jnp.ones((16, 128), BF)

    def wstep(j, _):
        sl = pl.ds(pl.multiple_of(j * 512, 512), 512)
        w = jnp.zeros((16, 512), F32)
        for part in split(wacc[sl, :], 3):
            w = w + lax.dot_general(ones, part.astype(BF), (((1,), (1,)), ((), ())), preferred_element_type=F32)
        wrow[:, sl] = w.astype(BF)
        return 0

    with jax.named_scope("weight"):
        lax.fori_loop(0, 8, wstep, 0)

    def bstep(j, _):
        ps = pl.ds(pl.multiple_of(j * NCHUNK, NCHUNK), NCHUNK)
        b = jnp.dot(wrow[...], jnp.abs(g_ref[:, ps]), preferred_element_type=F32)
        for q in range(NCHUNK // 128):
            bound_ref[j * (NCHUNK // 128) + q] = b[0:1, 128 * q : 128 * q + 128]
        return 0

    with jax.named_scope("bound"):
        lax.fori_loop(0, NPATCH // NCHUNK, bstep, 0)

    pair(bound_ref.at[pl.ds(16 * (1 - mc), 16)], bpair, 7).start()

    acc = jnp.zeros((NEP, 256), F32)
    for part in split(a_ref[...], 3):
        acc = acc + jnp.dot(part.astype(BF), design_b, preferred_element_type=F32)
    parts = split(acc, 2)
    pseudo = jnp.concatenate(parts, axis=0).astype(BF)
    with jax.named_scope("wait_ifg"):
        mine.wait()
        wait_got(got.at[pl.ds(1, DEV - 1)], 0)

    def sstep(k, _):
        sl = pl.ds(pl.multiple_of(k * 256, 256), 256)
        out = jnp.dot(pseudo, got[:, :, sl].reshape(256, 256), preferred_element_type=F32)
        ser = out[:NEP] + out[NEP:]
        series[:, sl] = ser
        high, low = split(ser, 2)
        resid[0:NEP, sl] = high.astype(BF)
        resid[NEP : 2 * NEP, sl] = low.astype(BF)
        return 0

    with jax.named_scope("series"):
        lax.fori_loop(0, 16, sstep, 0)

    with jax.named_scope("send_bound"):
        got_pair(bpair, 7)
        bsend[...] = bound_ref[pl.ds(16 * mc, 16)] + bpair[...]
        peers(lambda pp, half, xh: copy(bsend.at[pp], brecv.at[mine_at], 1, 2 * pp + half, 2 * xh + mc).start())
        brecv[mine_at] = bsend[mp // 2]

    def project(send, recv, psend, precv, k):
        def product(pc):
            out = jnp.dot(resid[...], g_ref[:, pl.ds(pl.multiple_of(pc * NCHUNK, NCHUNK), NCHUNK)], preferred_element_type=F32)
            return out[:NEP] + out[NEP:]

        def give(j, _):
            psend[j] = product(4 * (1 - mc) + j).astype(BF)

            @pl.when(j > 0)
            def _():
                pair(psend.at[j - 1], precv.at[j - 1], k + j - 1).start()

            return 0

        def push(j):
            ch = lax.rem(mp // 8 + j, 4)
            for q in range(4):
                for half in range(2):
                    pix = 2 * (4 * ch + q) + half
                    for xh in range(2):
                        eb = 2 * xh + half

                        @pl.when((pix != mp) | (mx != xh))
                        def _():
                            copy(send.at[4 * ch + q, eb], recv.at[mine_at], k + 4, pix, 2 * xh + mc).start()

        def keep(j, _):
            ch = lax.rem(mp // 8 + j, 4)
            rhs = product(4 * mc + ch)
            got_pair(precv.at[ch], k + ch)
            rhs = (rhs + precv[ch].astype(F32)).astype(BF)
            for q in range(4):
                for eb in range(4):
                    send[4 * ch + q, eb] = rhs[16 * eb : 16 * eb + 16, 128 * q : 128 * q + 128]

            @pl.when(j > 0)
            def _():
                push(j - 1)

            return 0

        with jax.named_scope("project"):
            lax.fori_loop(0, 4, give, 0)
            pair(psend.at[3], precv.at[3], k + 3).start()
            lax.fori_loop(0, 4, keep, 0)
            push(3)
        recv[mine_at] = send[mp // 2, eb_own]
        with jax.named_scope("wait_rhs"):
            wait_got(recv.at[pl.ds(1, PEERS - 1)], k + 4)
        return jnp.sum(recv[...].astype(F32), axis=0)

    def share(buf, i, k):
        with jax.named_scope("send_slip"):
            peers(lambda pp, half, xh: copy(own.at[i], buf.at[pb_own, eb_own], k, 2 * pp + half, 2 * xh + mc).start())
        buf[pb_own, eb_own] = own[i]
        with jax.named_scope("wait_slip"):
            wait_got(recv1.at[pl.ds(1, PEERS - 1)], k)
        half = pl.ds(16 * mc, 16)
        pair(buf.at[half], buf.at[half], k + 1).start()

    def spread(buf, core):
        for b in range(16):
            slipf[:, 128 * b : 128 * b + 128] = buf[16 * core + b].reshape(NEP, 128)

    def times_green(core, use):
        cols = pl.ds(pl.multiple_of(core * 2048, 2048), 2048)

        def one(j, _):
            gs = pl.ds(pl.multiple_of(j * NCHUNK, NCHUNK), NCHUNK)
            use(gs, lax.dot_general(slipf[...], g_ref[gs, cols], (((1,), (1,)), ((), ())), preferred_element_type=F32))
            return 0

        lax.fori_loop(0, PIX_DEV // NCHUNK, one, 0)

    rhs = project(send1, recv1, psend1, precv1, 8)
    wait_got(brecv.at[pl.ds(1, PEERS - 1)], 1)
    bound = jnp.sum(brecv[...], axis=0)
    slip = rhs / bound
    own[0] = slip.astype(BF)
    share(all1, 0, 2)

    def first(gs, out):
        series[:, gs] = series[:, gs] - out

    def second(gs, out):
        high, low = split(series[:, gs] - out, 2)
        resid[0:NEP, gs] = high.astype(BF)
        resid[NEP : 2 * NEP, gs] = low.astype(BF)

    with jax.named_scope("guess"):
        spread(all1, mc)
        times_green(mc, first)
    got_pair(all1.at[pl.ds(16 * (1 - mc), 16)], 3)
    with jax.named_scope("guess2"):
        spread(all1, 1 - mc)
        times_green(1 - mc, second)
    rhs = project(send2, recv2, psend2, precv2, 13)
    slip = slip + rhs / bound
    own[1] = slip.astype(BF)
    fine[...] = slip
    home = pb_own == mp
    for rep in range(REP):

        @pl.when(jnp.logical_not(home) | (mr != rep))
        def _():
            copy(fine, blk.at[eb_own], 6, pb_own, rep).start()

    share(all2, 1, 4)

    def third(gs, out):
        pred_ref[:, gs] = out

    def fourth(gs, out):
        pred_ref[:, gs] = pred_ref[:, gs] + out

    with jax.named_scope("final"):
        spread(all2, mc)
        times_green(mc, third)
    got_pair(all2.at[pl.ds(16 * (1 - mc), 16)], 5)
    with jax.named_scope("final2"):
        spread(all2, 1 - mc)
        times_green(1 - mc, fourth)

    @pl.when(home)
    def _():
        wait_got(blk.at[pl.ds(0, REP - 1)], 6)
        wait_sent(blk.at[pl.ds(0, REP - 1)], 6)
        blk[eb_own] = fine[...]

    @pl.when(jnp.logical_not(home))
    def _():
        wait_got(blk, 6)
        wait_sent(blk, 6)

    slip_ref[...] = pltpu.roll(blk[...].reshape(NEP, 128), lax.rem(128 - 32 * mr, 128), 1)
    wait_sent(got.at[pl.ds(1, DEV - 1)], 0)
    wait_sent(brecv.at[pl.ds(1, PEERS - 1)], 1)
    for k in (2, 4, 12, 17):
        wait_sent(recv1.at[pl.ds(1, PEERS - 1)], k)
    wait_sent(bpair, 7)
    for k in (3, 5):
        wait_sent(all1.at[pl.ds(0, 16)], k)
    for k in (8, 9, 10, 11, 13, 14, 15, 16):
        wait_sent(psend1.at[0], k)


def on_device(interferograms, epoch_pairs, los, patch_place, patch_depth):
    x = interferograms.astype(BF).reshape(2, DEV, PIX_DEV).transpose(1, 0, 2)
    vm = pl.BlockSpec(memory_space=pltpu.VMEM)
    predicted, slip = pl.pallas_call(
        kernel,
        out_shape=(jax.ShapeDtypeStruct((NEP, PIX_DEV), F32), jax.ShapeDtypeStruct((NEP, 128), F32)),
        in_specs=[pl.BlockSpec(memory_space=pl.ANY)] + [vm] * 4,
        out_specs=(vm, vm),
        scratch_shapes=[
            pltpu.VMEM((24, PIX_DEV), F32),
            pltpu.VMEM((24, NPATCH), F32),
            pltpu.VMEM((8, NPATCH), F32),
            pltpu.VMEM((8, NPATCH), F32),
            pltpu.VMEM((PIX_DEV, 128), F32),
            pltpu.VMEM((NEP, NEP), F32),
            pltpu.VMEM((PIX, 1, 128), F32),
            pltpu.VMEM((DEV, 2, PIX_DEV), BF),
            pltpu.VMEM((NEP, PIX_DEV), F32),
            pltpu.VMEM((16, REP) + CH, BF),
            pltpu.VMEM((16, REP) + CH, BF),
            pltpu.VMEM((PEERS,) + CH, BF),
            pltpu.VMEM((PEERS,) + CH, BF),
            pltpu.VMEM((4, NEP, NCHUNK), BF),
            pltpu.VMEM((4, NEP, NCHUNK), BF),
            pltpu.VMEM((4, NEP, NCHUNK), BF),
            pltpu.VMEM((4, NEP, NCHUNK), BF),
            pltpu.VMEM((16, 1, 128), F32),
            pltpu.VMEM((16, 1, 128), F32),
            pltpu.VMEM((PEERS, 1, 128), F32),
            pltpu.VMEM((2,) + CH, BF),
            pltpu.VMEM((PIX, REP) + CH, BF),
            pltpu.VMEM((PIX, REP) + CH, BF),
            pltpu.VMEM(CH, F32),
            pltpu.VMEM((REP,) + CH, F32),
            pltpu.SemaphoreType.DMA((18,)),
            pltpu.SemaphoreType.DMA((18,)),
            pltpu.SemaphoreType.DMA(()),
        ],
        compiler_params=pltpu.CompilerParams(vmem_limit_bytes=52 << 20, has_side_effects=True, collective_id=0),
        name="slip",
    )(x, epoch_pairs, los, patch_place, patch_depth.reshape(1, NPATCH))
    return predicted, slip[:, :32]


def solution(mesh):
    placed = (P(("pix", "rep"), None), P(), P(None, ("pix", "rep")), P(), P())
    return jax.shard_map(
        on_device,
        mesh=mesh,
        in_specs=placed,
        out_specs=(P(None, ("pix", "rep")), P(None, ("pix", "rep"))),
        check_vma=False,
    )
```

```python
import functools

import jax
import jax.numpy as jnp
from jax import lax
from jax.experimental import pallas as pl
from jax.experimental.pallas import tpu as pltpu
from jax.sharding import PartitionSpec as P

NEP = 64
NPATCH = 4096
PIX_DEV = 4096
IMG_W = 1024
PIX = 32
REP = 4
DEV = PIX * REP
F32, BF = jnp.float32, jnp.bfloat16
MESH = pl.DeviceIdType.MESH
damping = 0.5


def split(x, n):
    out = []
    for _ in range(n):
        h = x.astype(BF).astype(F32)
        out.append(h)
        x = x - h
    return out

CB, PB = 64, 1024
NCHUNK = 1024
GCHUNK = 1024
PEERS = DEV // 2
CH = (16, 128)


def features(los_ref, place_ref, depth_ref, pixrow, pixcol, patchrow, patchf, prow, srow):
    base = (lax.axis_index("pix") * REP + lax.axis_index("rep")).astype(F32)
    cx = place_ref[0:1, :].astype(F32)
    ny = place_ref[1:2, :].astype(F32)
    d2 = depth_ref[...].astype(F32) + 2.0
    px = cx * 8.0 + 4.0
    py = (ny - base) * 8.0 + 3.0
    h = d2 * 5.0
    prow[0:1, :] = px
    for r in range(4):
        dy = 2.0 * r - py
        srow[r : r + 1, :] = dy * dy + h * h
    f1 = split(d2 * (px - 1024.0), 2)
    f2 = split(d2 * py, 2)
    rows = [d2] * 3 + [-f1[0], -f1[1]] * 3 + [-f2[0], -f2[1]] * 3 + [d2 * h] * 3
    patchrow[...] = jnp.zeros_like(patchrow)
    for k, v in enumerate(rows):
        patchrow[k : k + 1, :] = v
    patchf[...] = patchrow[...].astype(BF)
    g = lax.broadcasted_iota(jnp.int32, (1, PIX_DEV), 1)
    xc = ((g % IMG_W) * 2 + (1 - 1024)).astype(F32)
    yc = ((g // IMG_W) * 2).astype(F32)
    l0 = los_ref[0:1, :] * 100.0
    l1 = los_ref[1:2, :] * 100.0
    l2 = los_ref[2:3, :] * 100.0
    a = split(l0 * xc + l1 * yc, 3)
    s0, s1, s2 = split(l0, 3), split(l1, 3), split(l2, 3)
    rows = a + [s0[0], s0[0], s0[1], s0[1], s0[2], s0[2]] + [s1[0], s1[0], s1[1], s1[1], s1[2], s1[2]] + s2
    pixrow[...] = jnp.zeros_like(pixrow)
    for k, v in enumerate(rows):
        pixrow[k : k + 1, :] = v
    pixcol[...] = pixrow[...].T.astype(BF)


def invert_step(k, a_ref):
    a = a_ref[...]
    kk = lax.rem(k, NEP)
    lane = lax.broadcasted_iota(jnp.int32, (NEP, NEP), 1)
    sub = lax.broadcasted_iota(jnp.int32, (NEP, NEP), 0)
    row = a_ref[pl.ds(kk, 1), :]
    lane1 = lax.broadcasted_iota(jnp.int32, (1, NEP), 1)
    inv = 1.0 / jnp.sum(jnp.where(lane1 == kk, row, 0.0), axis=1, keepdims=True)
    col = jnp.sum(jnp.where(lane == kk, a, 0.0), axis=1, keepdims=True)
    new_row = jnp.where(lane1 == kk, inv, row * inv)
    rest = jnp.where(lane == kk, 0.0, a) - col * new_row
    new = jnp.where(sub == kk, new_row, rest)
    a_ref[...] = jnp.where(k < NEP, new, a)


def for_others(mp, mr, fn):
    for i in range(1, REP):
        fn(mp, lax.rem(mr + i, REP))

    def one(k, _):
        pix = lax.rem(mp + k, PIX)
        for rep in range(REP):
            fn(pix, rep)
        return 0

    lax.fori_loop(1, PIX, one, 0)


def opening(x_ref, xb, lsem, xf):
    load = pltpu.make_async_copy(x_ref, xf, lsem)
    load.start()
    ready = pltpu.get_barrier_semaphore()

    def tell(pix, rep):
        pl.semaphore_signal(ready, inc=1, device_id={"pix": pix, "rep": rep}, device_id_type=MESH)

    with jax.named_scope("signal"):
        for_others(lax.axis_index("pix"), lax.axis_index("rep"), tell)
    load.wait()

    def one(k, _):
        for u in range(4):
            xb[4 * k + u] = xf[:, pl.ds(pl.multiple_of((4 * k + u) * PIX_DEV, PIX_DEV), PIX_DEV)].astype(BF)
        return 0

    with jax.named_scope("convert"):
        lax.fori_loop(0, DEV // 4, one, 0)


def kernel(*refs):
    pl.run_scoped(functools.partial(opening, refs[0], refs[7], refs[-1]), pltpu.VMEM((2, DEV * PIX_DEV), F32))
    pl.run_scoped(
        functools.partial(body, *refs),
        pltpu.VMEM((PIX_DEV, NPATCH), BF),
        pltpu.VMEM((PIX_DEV, 24), BF),
        pltpu.VMEM((24, NPATCH), BF),
        pltpu.VMEM((16, PIX_DEV), BF),
        pltpu.VMEM((2 * NEP, PIX_DEV), BF),
        pltpu.VMEM((NEP, NPATCH // 2), BF),
    )


def body(
    x_ref, pairs_ref, los_ref, place_ref, depth_ref, pred_ref, slip_ref,
    xb, pixrow, patchrow, prow, srow, wacc, a_ref, bound_ref,
    got, series, send1, send2, recv1, recv2, psend1, psend2, precv1, precv2, bpair, bsend, brecv, own, all1, all2, fine, blk,
    ssem, rsem, lsem,
    g_ref, pixcol, patchf, wrow, resid, slipf,
):
    mp, mr = lax.axis_index("pix"), lax.axis_index("rep")
    me = mp * REP + mr

    def copy(src, dst, k, pix, rep):
        return pltpu.make_async_remote_copy(src, dst, ssem.at[k], rsem.at[k], device_id={"pix": pix, "rep": rep}, device_id_type=MESH)

    def wait_sent(buf, k):
        pltpu.make_async_copy(buf, buf, ssem.at[k]).wait()

    def wait_got(buf, k):
        pltpu.make_async_copy(buf, buf, rsem.at[k]).wait()

    others = functools.partial(for_others, mp, mr)

    mc, mx = lax.rem(mr, 2), mr // 2
    mine_at = 2 * mp + mx
    pb_own, eb_own = 16 * mc + mp // 2, 2 * mx + lax.rem(mp, 2)

    def pair(src, dst, k):
        return copy(src, dst, k, mp, mr + 1 - 2 * mc)

    got_pair = wait_got

    def peers(fn):
        for i in range(1, 4):
            at = lax.rem(2 * lax.rem(mp, 2) + mx + i, 4)
            fn(mp // 2, at // 2, lax.rem(at, 2))

        def one(k, _):
            pp = lax.rem(mp // 2 + k, 16)
            for half in range(2):
                for xh in range(2):
                    fn(pp, half, xh)
            return 0

        lax.fori_loop(1, 16, one, 0)

    with jax.named_scope("features"):
        features(los_ref, place_ref, depth_ref, pixrow, pixcol, patchrow, patchf, prow, srow)
    with jax.named_scope("wait_ready"):
        pl.semaphore_wait(pltpu.get_barrier_semaphore(), DEV - 1)

    with jax.named_scope("send_ifg"):
        others(lambda pix, rep: copy(xb.at[pix * REP + rep], got.at[me], 0, pix, rep).start())
        got[me] = xb[me]

    with jax.named_scope("normal"):
        epoch = lax.broadcasted_iota(jnp.int32, (NEP, 256), 0)
        design_t = (epoch == pairs_ref[1:2, :]).astype(F32) - (epoch == pairs_ref[0:1, :]).astype(F32)
        design_b = design_t.astype(BF)
        normal = lax.dot_general(design_b, design_b, (((1,), (1,)), ((), ())), preferred_element_type=F32)
        eye = lax.broadcasted_iota(jnp.int32, (NEP, NEP), 0) == lax.broadcasted_iota(jnp.int32, (NEP, NEP), 1)
        a_ref[...] = normal + jnp.where(eye, damping, 0.0)
        wacc[...] = jnp.zeros_like(wacc)

    def step(it, _):
        invert_step(it, a_ref)
        c0 = pl.multiple_of((it // (NPATCH // PB)) * CB, CB)
        p0 = pl.multiple_of(lax.rem(it, NPATCH // PB) * PB, PB)
        xs = (lax.broadcasted_iota(jnp.int32, (CB, 128), 0) * 2 + (2 * c0 + 1)).astype(F32)
        dxs = []
        for q in range(PB // 128):
            dx = xs - prow[0:1, pl.ds(pl.multiple_of(p0 + 128 * q, 128), 128)]
            dxs.append(dx * dx)
        for r in range(4):
            rowsl = pl.ds(pl.multiple_of(r * IMG_W + c0, CB), CB)
            t = jnp.dot(pixcol[rowsl, :], patchf[:, pl.ds(p0, PB)], preferred_element_type=F32)
            acc = wacc[rowsl, :]
            mags = []
            for q in range(PB // 128):
                ps = pl.ds(pl.multiple_of(p0 + 128 * q, 128), 128)
                inv = lax.rsqrt(dxs[q] + srow[r : r + 1, ps])
                gf = (t[:, 128 * q : 128 * q + 128] * (inv * inv * inv)).astype(BF)
                g_ref[rowsl, ps] = gf
                mags.append(jnp.abs(gf))
            while len(mags) > PB // 512:
                mags = [a + b for a, b in zip(mags[0::2], mags[1::2])]
            for m in mags:
                acc = acc + m.astype(F32)
            wacc[rowsl, :] = acc
        return 0

    with jax.named_scope("green"):
        lax.fori_loop(0, (IMG_W // CB) * (NPATCH // PB), step, 0)

    ones = jnp.ones((16, 128), BF)

    def wstep(j, _):
        sl = pl.ds(pl.multiple_of(j * 2048, 2048), 2048)
        w = jnp.zeros((16, 2048), F32)
        for part in split(wacc[sl, :], 3):
            w = w + lax.dot_general(ones, part.astype(BF), (((1,), (1,)), ((), ())), preferred_element_type=F32)
        wrow[:, sl] = w.astype(BF)
        return 0

    with jax.named_scope("weight"):
        lax.fori_loop(0, 2, wstep, 0)

    def bstep(j, _):
        ps = pl.ds(pl.multiple_of(j * 512, 512), 512)
        b = jnp.dot(wrow[...], jnp.abs(g_ref[:, ps]), preferred_element_type=F32)
        for q in range(4):
            bound_ref[4 * j + q] = b[0:1, 128 * q : 128 * q + 128]
        return 0

    with jax.named_scope("bound"):
        lax.fori_loop(0, 8, bstep, 0)

    pair(bound_ref.at[pl.ds(16 * (1 - mc), 16)], bpair, 7).start()

    acc = jnp.zeros((NEP, 256), F32)
    for part in split(a_ref[...], 3):
        acc = acc + jnp.dot(part.astype(BF), design_b, preferred_element_type=F32)
    parts = split(acc, 2)
    pseudo = jnp.concatenate(parts, axis=0).astype(BF)
    with jax.named_scope("wait_ifg"):
        wait_got(got.at[pl.ds(1, DEV - 1)], 0)

    def sstep(k, _):
        sl = pl.ds(pl.multiple_of(k * 512, 512), 512)
        out = jnp.dot(pseudo, got[:, :, sl].reshape(256, 512), preferred_element_type=F32)
        ser = out[:NEP] + out[NEP:]
        series[:, sl] = ser
        high, low = split(ser, 2)
        resid[0:NEP, sl] = high.astype(BF)
        resid[NEP : 2 * NEP, sl] = low.astype(BF)
        return 0

    with jax.named_scope("series"):
        lax.fori_loop(0, 8, sstep, 0)

    with jax.named_scope("send_bound"):
        got_pair(bpair, 7)
        bsend[...] = bound_ref[pl.ds(16 * mc, 16)] + bpair[...]
        peers(lambda pp, half, xh: copy(bsend.at[pp], brecv.at[mine_at], 1, 2 * pp + half, 2 * xh + mc).start())
        brecv[mine_at] = bsend[mp // 2]

    def project(send, recv, psend, precv, k):
        def product(pc):
            out = jnp.dot(resid[...], g_ref[:, pl.ds(pl.multiple_of(pc * NCHUNK, NCHUNK), NCHUNK)], preferred_element_type=F32)
            return out[:NEP] + out[NEP:]

        def push(ch, near):
            for q in range(8):
                for half in range(2):
                    pix = 2 * (8 * ch + q) + half
                    for xh in range(2):

                        def go():
                            copy(send.at[8 * ch + q, 2 * xh + half], recv.at[mine_at], k + 2, pix, 2 * xh + mc).start()

                        if near:
                            pl.when((pix != mp) | (mx != xh))(go)
                        else:
                            go()

        def keep(ch):
            rhs = product(2 * mc + ch)
            got_pair(precv.at[ch], k + ch)
            rhs = (rhs + precv[ch].astype(F32)).astype(BF)
            for q in range(8):
                for eb in range(4):
                    send[8 * ch + q, eb] = rhs[16 * eb : 16 * eb + 16, 128 * q : 128 * q + 128]

        with jax.named_scope("give"):
            for j in range(2):
                psend[j] = product(2 * (1 - mc) + j).astype(BF)
                pair(psend.at[j], precv.at[j], k + j).start()
        with jax.named_scope("keep"):
            own_ch = mp // 16
            keep(1 - own_ch)
            push(1 - own_ch, False)
            keep(own_ch)
            push(own_ch, True)
        recv[mine_at] = send[mp // 2, eb_own]
        with jax.named_scope("wait_rhs"):
            wait_got(recv.at[pl.ds(1, PEERS - 1)], k + 2)
        return jnp.sum(recv[...].astype(F32), axis=0)

    def share(buf, i, k):
        with jax.named_scope("send_slip"):
            peers(lambda pp, half, xh: copy(own.at[i], buf.at[pb_own, eb_own], k, 2 * pp + half, 2 * xh + mc).start())
        buf[pb_own, eb_own] = own[i]
        with jax.named_scope("wait_slip"):
            wait_got(recv1.at[pl.ds(1, PEERS - 1)], k)
        half = pl.ds(16 * mc, 16)
        pair(buf.at[half], buf.at[half], k + 1).start()

    def spread(buf, core):
        for b in range(16):
            slipf[:, 128 * b : 128 * b + 128] = buf[16 * core + b].reshape(NEP, 128)

    def times_green(core, use):
        cols = pl.ds(pl.multiple_of(core * 2048, 2048), 2048)

        def one(j, _):
            gs = pl.ds(pl.multiple_of(j * GCHUNK, GCHUNK), GCHUNK)
            use(gs, lax.dot_general(slipf[...], g_ref[gs, cols], (((1,), (1,)), ((), ())), preferred_element_type=F32))
            return 0

        lax.fori_loop(0, PIX_DEV // GCHUNK, one, 0)

    rhs = project(send1, recv1, psend1, precv1, 8)
    wait_got(brecv.at[pl.ds(1, PEERS - 1)], 1)
    bound = jnp.sum(brecv[...], axis=0)
    slip = rhs / bound
    own[0] = slip.astype(BF)
    share(all1, 0, 2)

    def first(gs, out):
        series[:, gs] = series[:, gs] - out

    def second(gs, out):
        high, low = split(series[:, gs] - out, 2)
        resid[0:NEP, gs] = high.astype(BF)
        resid[NEP : 2 * NEP, gs] = low.astype(BF)

    with jax.named_scope("guess"):
        spread(all1, mc)
        times_green(mc, first)
    got_pair(all1.at[pl.ds(16 * (1 - mc), 16)], 3)
    with jax.named_scope("guess2"):
        spread(all1, 1 - mc)
        times_green(1 - mc, second)
    rhs = project(send2, recv2, psend2, precv2, 11)
    slip = slip + rhs / bound
    own[1] = slip.astype(BF)
    fine[...] = slip
    home = pb_own == mp
    for rep in range(REP):

        @pl.when(jnp.logical_not(home) | (mr != rep))
        def _():
            copy(fine, blk.at[eb_own], 6, pb_own, rep).start()

    share(all2, 1, 4)

    def third(gs, out):
        pred_ref[:, gs] = out

    def fourth(gs, out):
        pred_ref[:, gs] = pred_ref[:, gs] + out

    with jax.named_scope("final"):
        spread(all2, mc)
        times_green(mc, third)
    got_pair(all2.at[pl.ds(16 * (1 - mc), 16)], 5)
    with jax.named_scope("final2"):
        spread(all2, 1 - mc)
        times_green(1 - mc, fourth)

    @pl.when(home)
    def _():
        wait_got(blk.at[pl.ds(0, REP - 1)], 6)
        wait_sent(blk.at[pl.ds(0, REP - 1)], 6)
        blk[eb_own] = fine[...]

    @pl.when(jnp.logical_not(home))
    def _():
        wait_got(blk, 6)
        wait_sent(blk, 6)

    slip_ref[...] = pltpu.roll(blk[...].reshape(NEP, 128), lax.rem(128 - 32 * mr, 128), 1)
    wait_sent(got.at[pl.ds(1, DEV - 1)], 0)
    wait_sent(brecv.at[pl.ds(1, PEERS - 1)], 1)
    for k in (2, 4, 10, 13):
        wait_sent(recv1.at[pl.ds(1, PEERS - 1)], k)
    wait_sent(bpair, 7)
    for k in (3, 5):
        wait_sent(all1.at[pl.ds(0, 16)], k)
    for k in (8, 9, 11, 12):
        wait_sent(psend1.at[0], k)


def on_device(interferograms, epoch_pairs, los, patch_place, patch_depth):
    vm = pl.BlockSpec(memory_space=pltpu.VMEM)
    predicted, slip = pl.pallas_call(
        kernel,
        out_shape=(jax.ShapeDtypeStruct((NEP, PIX_DEV), F32), jax.ShapeDtypeStruct((NEP, 128), F32)),
        in_specs=[pl.BlockSpec(memory_space=pl.ANY)] + [vm] * 4,
        out_specs=(vm, vm),
        scratch_shapes=[
            pltpu.VMEM((DEV, 2, PIX_DEV), BF),
            pltpu.VMEM((24, PIX_DEV), F32),
            pltpu.VMEM((24, NPATCH), F32),
            pltpu.VMEM((8, NPATCH), F32),
            pltpu.VMEM((8, NPATCH), F32),
            pltpu.VMEM((PIX_DEV, 128), F32),
            pltpu.VMEM((NEP, NEP), F32),
            pltpu.VMEM((PIX, 1, 128), F32),
            pltpu.VMEM((DEV, 2, PIX_DEV), BF),
            pltpu.VMEM((NEP, PIX_DEV), F32),
            pltpu.VMEM((16, REP) + CH, BF),
            pltpu.VMEM((16, REP) + CH, BF),
            pltpu.VMEM((PEERS,) + CH, BF),
            pltpu.VMEM((PEERS,) + CH, BF),
            pltpu.VMEM((2, NEP, NCHUNK), BF),
            pltpu.VMEM((2, NEP, NCHUNK), BF),
            pltpu.VMEM((2, NEP, NCHUNK), BF),
            pltpu.VMEM((2, NEP, NCHUNK), BF),
            pltpu.VMEM((16, 1, 128), F32),
            pltpu.VMEM((16, 1, 128), F32),
            pltpu.VMEM((PEERS, 1, 128), F32),
            pltpu.VMEM((2,) + CH, BF),
            pltpu.VMEM((PIX, REP) + CH, BF),
            pltpu.VMEM((PIX, REP) + CH, BF),
            pltpu.VMEM(CH, F32),
            pltpu.VMEM((REP,) + CH, F32),
            pltpu.SemaphoreType.DMA((14,)),
            pltpu.SemaphoreType.DMA((14,)),
            pltpu.SemaphoreType.DMA(()),
        ],
        compiler_params=pltpu.CompilerParams(vmem_limit_bytes=60 << 20, has_side_effects=True, collective_id=0),
        name="slip",
    )(interferograms, epoch_pairs, los, patch_place, patch_depth.reshape(1, NPATCH))
    return predicted, slip[:, :32]


def solution(mesh):
    placed = (P(("pix", "rep"), None), P(), P(None, ("pix", "rep")), P(), P())
    return jax.shard_map(
        on_device,
        mesh=mesh,
        in_specs=placed,
        out_specs=(P(None, ("pix", "rep")), P(None, ("pix", "rep"))),
        check_vma=False,
    )
```

```python
import functools

import jax
import jax.numpy as jnp
from jax import lax
from jax.experimental import pallas as pl
from jax.experimental.pallas import tpu as pltpu
from jax.sharding import PartitionSpec as P

NEP = 64
NPATCH = 4096
PIX_DEV = 4096
IMG_W = 1024
PIX = 32
REP = 4
DEV = PIX * REP
F32, BF = jnp.float32, jnp.bfloat16
MESH = pl.DeviceIdType.MESH
damping = 0.5


def split(x, n):
    out = []
    for _ in range(n):
        h = x.astype(BF).astype(F32)
        out.append(h)
        x = x - h
    return out

CB, PB = 64, 2048
NCHUNK = 1024
GCHUNK = 2048
PEERS = DEV // 2
CH = (16, 128)


def features(los_ref, place_ref, depth_ref, pixrow, pixcol, patchrow, patchf, prow, srow):
    base = (lax.axis_index("pix") * REP + lax.axis_index("rep")).astype(F32)
    cx = place_ref[0:1, :].astype(F32)
    ny = place_ref[1:2, :].astype(F32)
    d2 = depth_ref[...].astype(F32) + 2.0
    px = cx * 8.0 + 4.0
    py = (ny - base) * 8.0 + 3.0
    h = d2 * 5.0
    prow[0:1, :] = px
    for r in range(4):
        dy = 2.0 * r - py
        srow[r : r + 1, :] = dy * dy + h * h
    f1 = split(d2 * (px - 1024.0), 2)
    f2 = split(d2 * py, 2)
    rows = [d2] * 3 + [-f1[0], -f1[1]] * 3 + [-f2[0], -f2[1]] * 3 + [d2 * h] * 3
    patchrow[...] = jnp.zeros_like(patchrow)
    for k, v in enumerate(rows):
        patchrow[k : k + 1, :] = v
    patchf[...] = patchrow[...].astype(BF)
    g = lax.broadcasted_iota(jnp.int32, (1, PIX_DEV), 1)
    xc = ((g % IMG_W) * 2 + (1 - 1024)).astype(F32)
    yc = ((g // IMG_W) * 2).astype(F32)
    l0 = los_ref[0:1, :] * 100.0
    l1 = los_ref[1:2, :] * 100.0
    l2 = los_ref[2:3, :] * 100.0
    a = split(l0 * xc + l1 * yc, 3)
    s0, s1, s2 = split(l0, 3), split(l1, 3), split(l2, 3)
    rows = a + [s0[0], s0[0], s0[1], s0[1], s0[2], s0[2]] + [s1[0], s1[0], s1[1], s1[1], s1[2], s1[2]] + s2
    pixrow[...] = jnp.zeros_like(pixrow)
    for k, v in enumerate(rows):
        pixrow[k : k + 1, :] = v
    pixcol[...] = pixrow[...].T.astype(BF)


def invert_step(k, a_ref):
    a = a_ref[...]
    kk = lax.rem(k, NEP)
    lane = lax.broadcasted_iota(jnp.int32, (NEP, NEP), 1)
    sub = lax.broadcasted_iota(jnp.int32, (NEP, NEP), 0)
    row = a_ref[pl.ds(kk, 1), :]
    lane1 = lax.broadcasted_iota(jnp.int32, (1, NEP), 1)
    inv = 1.0 / jnp.sum(jnp.where(lane1 == kk, row, 0.0), axis=1, keepdims=True)
    col = jnp.sum(jnp.where(lane == kk, a, 0.0), axis=1, keepdims=True)
    new_row = jnp.where(lane1 == kk, inv, row * inv)
    rest = jnp.where(lane == kk, 0.0, a) - col * new_row
    new = jnp.where(sub == kk, new_row, rest)
    a_ref[...] = jnp.where(k < NEP, new, a)


def for_others(mp, mr, fn):
    for i in range(1, REP):
        fn(mp, lax.rem(mr + i, REP))

    def one(k, _):
        pix = lax.rem(mp + 13 * k, PIX)
        for rep in range(REP):
            fn(pix, rep)
        return 0

    lax.fori_loop(1, PIX, one, 0)


def opening(inputs, places, lsem, xf):
    xb = places[4]
    loads = [pltpu.make_async_copy(src, dst, lsem.at[i]) for i, (src, dst) in enumerate(zip(inputs, (xf,) + tuple(places[:4])))]
    for load in loads:
        load.start()
    ready = pltpu.get_barrier_semaphore()

    def tell(pix, rep):
        pl.semaphore_signal(ready, inc=1, device_id={"pix": pix, "rep": rep}, device_id_type=MESH)

    with jax.named_scope("signal"):
        for_others(lax.axis_index("pix"), lax.axis_index("rep"), tell)
    for load in loads:
        load.wait()

    def one(k, _):
        for u in range(4):
            xb[4 * k + u] = xf[:, pl.ds(pl.multiple_of((4 * k + u) * PIX_DEV, PIX_DEV), PIX_DEV)].astype(BF)
        return 0

    with jax.named_scope("convert"):
        lax.fori_loop(0, DEV // 4, one, 0)


def kernel(*refs):
    pl.run_scoped(functools.partial(opening, refs[:5], refs[7:12], refs[-1]), pltpu.VMEM((2, DEV * PIX_DEV), F32))
    pl.run_scoped(functools.partial(body, *refs), pltpu.VMEM((PIX_DEV, NPATCH), BF))


def body(
    x_hbm, pairs_hbm, los_hbm, place_hbm, depth_hbm, pred_ref, slip_ref,
    pairs_ref, los_ref, place_ref, depth_ref, xb, a_ref, bound_ref,
    got, send1, send2, recv1, recv2, psend1, psend2, precv1, precv2, bpair, bsend, brecv, own, all1, all2, fine, blk,
    ssem, rsem, lsem,
    g_ref,
):
    mp, mr = lax.axis_index("pix"), lax.axis_index("rep")
    me = mp * REP + mr

    def copy(src, dst, k, pix, rep):
        return pltpu.make_async_remote_copy(src, dst, ssem.at[k], rsem.at[k], device_id={"pix": pix, "rep": rep}, device_id_type=MESH)

    def wait_sent(buf, k):
        pltpu.make_async_copy(buf, buf, ssem.at[k]).wait()

    def wait_got(buf, k):
        pltpu.make_async_copy(buf, buf, rsem.at[k]).wait()

    others = functools.partial(for_others, mp, mr)

    mc, mx = lax.rem(mr, 2), mr // 2
    mine_at = 2 * mp + mx
    pb_own, eb_own = 16 * mc + mp // 2, 2 * mx + lax.rem(mp, 2)

    def pair(src, dst, k):
        return copy(src, dst, k, mp, mr + 1 - 2 * mc)

    got_pair = wait_got

    def peers(fn):
        for i in range(1, 4):
            at = lax.rem(2 * lax.rem(mp, 2) + mx + i, 4)
            fn(mp // 2, at // 2, lax.rem(at, 2))

        def one(k, _):
            pp = lax.rem(mp // 2 + 7 * k, 16)
            for half in range(2):
                for xh in range(2):
                    fn(pp, half, xh)
            return 0

        lax.fori_loop(1, 16, one, 0)

    def design():
        epoch = lax.broadcasted_iota(jnp.int32, (NEP, 256), 0)
        return ((epoch == pairs_ref[1:2, :]).astype(F32) - (epoch == pairs_ref[0:1, :]).astype(F32)).astype(BF)

    def build(pixrow, patchrow, prow, srow, wacc, pixcol, patchf, wrow):
        with jax.named_scope("features"):
            features(los_ref, place_ref, depth_ref, pixrow, pixcol, patchrow, patchf, prow, srow)
        with jax.named_scope("wait_ready"):
            pl.semaphore_wait(pltpu.get_barrier_semaphore(), DEV - 1)

        with jax.named_scope("send_ifg"):
            others(lambda pix, rep: copy(xb.at[pix * REP + rep], got.at[me], 0, pix, rep).start())
            got[me] = xb[me]

        with jax.named_scope("normal"):
            design_b = design()
            normal = lax.dot_general(design_b, design_b, (((1,), (1,)), ((), ())), preferred_element_type=F32)
            eye = lax.broadcasted_iota(jnp.int32, (NEP, NEP), 0) == lax.broadcasted_iota(jnp.int32, (NEP, NEP), 1)
            a_ref[...] = normal + jnp.where(eye, damping, 0.0)
            wacc[...] = jnp.zeros_like(wacc)

        def step(it, _):
            invert_step(2 * it, a_ref)
            invert_step(2 * it + 1, a_ref)
            c0 = pl.multiple_of((it // (NPATCH // PB)) * CB, CB)
            p0 = pl.multiple_of(lax.rem(it, NPATCH // PB) * PB, PB)
            xs = (lax.broadcasted_iota(jnp.int32, (CB, 128), 0) * 2 + (2 * c0 + 1)).astype(F32)
            dxs = []
            for q in range(PB // 128):
                dx = xs - prow[0:1, pl.ds(pl.multiple_of(p0 + 128 * q, 128), 128)]
                dxs.append(dx * dx)
            for r in range(4):
                rowsl = pl.ds(pl.multiple_of(r * IMG_W + c0, CB), CB)
                t = jnp.dot(pixcol[rowsl, :], patchf[:, pl.ds(p0, PB)], preferred_element_type=F32)
                acc = wacc[rowsl, :]
                mags = []
                for q in range(PB // 128):
                    ps = pl.ds(pl.multiple_of(p0 + 128 * q, 128), 128)
                    inv = lax.rsqrt(dxs[q] + srow[r : r + 1, ps])
                    gf = (t[:, 128 * q : 128 * q + 128] * (inv * inv * inv)).astype(BF)
                    g_ref[rowsl, ps] = gf
                    mags.append(jnp.abs(gf))
                while len(mags) > PB // 512:
                    mags = [a + b for a, b in zip(mags[0::2], mags[1::2])]
                for m in mags:
                    acc = acc + m.astype(F32)
                wacc[rowsl, :] = acc
            return 0

        with jax.named_scope("green"):
            lax.fori_loop(0, (IMG_W // CB) * (NPATCH // PB), step, 0)

        ones = jnp.ones((16, 128), BF)

        def wstep(j, _):
            sl = pl.ds(pl.multiple_of(j * 2048, 2048), 2048)
            w = jnp.zeros((16, 2048), F32)
            for part in split(wacc[sl, :], 3):
                w = w + lax.dot_general(ones, part.astype(BF), (((1,), (1,)), ((), ())), preferred_element_type=F32)
            wrow[:, sl] = w.astype(BF)
            return 0

        with jax.named_scope("weight"):
            lax.fori_loop(0, 2, wstep, 0)

        def bstep(j, _):
            ps = pl.ds(pl.multiple_of(j * 1024, 1024), 1024)
            b = jnp.dot(wrow[...], jnp.abs(g_ref[:, ps]), preferred_element_type=F32)
            for q in range(8):
                bound_ref[8 * j + q] = b[0:1, 128 * q : 128 * q + 128]
            return 0

        with jax.named_scope("bound"):
            lax.fori_loop(0, 4, bstep, 0)

    pl.run_scoped(
        build,
        pltpu.VMEM((24, PIX_DEV), F32),
        pltpu.VMEM((24, NPATCH), F32),
        pltpu.VMEM((8, NPATCH), F32),
        pltpu.VMEM((8, NPATCH), F32),
        pltpu.VMEM((PIX_DEV, 128), F32),
        pltpu.VMEM((PIX_DEV, 24), BF),
        pltpu.VMEM((24, NPATCH), BF),
        pltpu.VMEM((16, PIX_DEV), BF),
    )

    def solve(series, resid, slipf):
        pair(bound_ref.at[pl.ds(16 * (1 - mc), 16)], bpair, 7).start()

        design_b = design()
        acc = jnp.zeros((NEP, 256), F32)
        for part in split(a_ref[...], 3):
            acc = acc + jnp.dot(part.astype(BF), design_b, preferred_element_type=F32)
        parts = split(acc, 2)
        pseudo = jnp.concatenate(parts, axis=0).astype(BF)
        with jax.named_scope("wait_ifg"):
            wait_got(got.at[pl.ds(1, DEV - 1)], 0)

        def sstep(k, _):
            sl = pl.ds(pl.multiple_of(k * 512, 512), 512)
            out = jnp.dot(pseudo, got[:, :, sl].reshape(256, 512), preferred_element_type=F32)
            ser = out[:NEP] + out[NEP:]
            series[:, sl] = ser
            high, low = split(ser, 2)
            resid[0:NEP, sl] = high.astype(BF)
            resid[NEP : 2 * NEP, sl] = low.astype(BF)
            return 0

        with jax.named_scope("series"):
            lax.fori_loop(0, 8, sstep, 0)

        with jax.named_scope("send_bound"):
            got_pair(bpair, 7)
            bsend[...] = bound_ref[pl.ds(16 * mc, 16)] + bpair[...]
            peers(lambda pp, half, xh: copy(bsend.at[pp], brecv.at[mine_at], 1, 2 * pp + half, 2 * xh + mc).start())
            brecv[mine_at] = bsend[mp // 2]

        def project(send, recv, psend, precv, k):
            def product(pc):
                parts = []
                for q in range(NCHUNK // 512):
                    cols = pl.ds(pl.multiple_of(pc * NCHUNK + 512 * q, 512), 512)
                    out = jnp.dot(resid[...], g_ref[:, cols], preferred_element_type=F32)
                    parts.append(out[:NEP] + out[NEP:])
                return jnp.concatenate(parts, axis=1)

            def push(ch, near):
                for q in range(8):
                    for half in range(2):
                        pix = 2 * (8 * ch + q) + half
                        for xh in range(2):

                            def go():
                                copy(send.at[8 * ch + q, 2 * xh + half], recv.at[mine_at], k + 2, pix, 2 * xh + mc).start()

                            if near:
                                pl.when((pix != mp) | (mx != xh))(go)
                            else:
                                go()

            def keep(ch):
                rhs = product(2 * mc + ch)
                got_pair(precv.at[ch], k + ch)
                rhs = (rhs + precv[ch].astype(F32)).astype(BF)
                for q in range(8):
                    for eb in range(4):
                        send[8 * ch + q, eb] = rhs[16 * eb : 16 * eb + 16, 128 * q : 128 * q + 128]

            with jax.named_scope("give"):
                for j in range(2):
                    psend[j] = product(2 * (1 - mc) + j).astype(BF)
                    pair(psend.at[j], precv.at[j], k + j).start()
            with jax.named_scope("keep"):
                own_ch = mp // 16
                keep(1 - own_ch)
                push(1 - own_ch, False)
                keep(own_ch)
                push(own_ch, True)
            recv[mine_at] = send[mp // 2, eb_own]
            with jax.named_scope("wait_rhs"):
                wait_got(recv.at[pl.ds(1, PEERS - 1)], k + 2)
            return jnp.sum(recv[...].astype(F32), axis=0)

        def share(buf, i, k):
            with jax.named_scope("send_slip"):
                peers(lambda pp, half, xh: copy(own.at[i], buf.at[pb_own, eb_own], k, 2 * pp + half, 2 * xh + mc).start())
            buf[pb_own, eb_own] = own[i]
            with jax.named_scope("wait_slip"):
                wait_got(recv1.at[pl.ds(1, PEERS - 1)], k)
            half = pl.ds(16 * mc, 16)
            pair(buf.at[half], buf.at[half], k + 1).start()

        def spread(buf, core):
            for b in range(16):
                slipf[:, 128 * b : 128 * b + 128] = buf[16 * core + b].reshape(NEP, 128)

        def times_green(core, use):
            cols = pl.ds(pl.multiple_of(core * 2048, 2048), 2048)

            def one(j, _):
                gs = pl.ds(pl.multiple_of(j * GCHUNK, GCHUNK), GCHUNK)
                use(gs, lax.dot_general(slipf[...], g_ref[gs, cols], (((1,), (1,)), ((), ())), preferred_element_type=F32))
                return 0

            lax.fori_loop(0, PIX_DEV // GCHUNK, one, 0)

        rhs = project(send1, recv1, psend1, precv1, 8)
        wait_got(brecv.at[pl.ds(1, PEERS - 1)], 1)
        bound = jnp.sum(brecv[...], axis=0)
        slip = rhs / bound
        own[0] = slip.astype(BF)
        share(all1, 0, 2)

        def first(gs, out):
            series[:, gs] = series[:, gs] - out

        def second(gs, out):
            high, low = split(series[:, gs] - out, 2)
            resid[0:NEP, gs] = high.astype(BF)
            resid[NEP : 2 * NEP, gs] = low.astype(BF)

        with jax.named_scope("guess"):
            spread(all1, mc)
            times_green(mc, first)
        got_pair(all1.at[pl.ds(16 * (1 - mc), 16)], 3)
        with jax.named_scope("guess2"):
            spread(all1, 1 - mc)
            times_green(1 - mc, second)
        rhs = project(send2, recv2, psend2, precv2, 11)
        slip = slip + rhs / bound
        own[1] = slip.astype(BF)
        fine[...] = slip
        home = pb_own == mp
        for rep in range(REP):

            @pl.when(jnp.logical_not(home) | (mr != rep))
            def _():
                copy(fine, blk.at[eb_own], 6, pb_own, rep).start()

        share(all2, 1, 4)

        def third(gs, out):
            pred_ref[:, gs] = out

        def fourth(gs, out):
            pred_ref[:, gs] = pred_ref[:, gs] + out

        with jax.named_scope("final"):
            spread(all2, mc)
            times_green(mc, third)
        got_pair(all2.at[pl.ds(16 * (1 - mc), 16)], 5)
        with jax.named_scope("final2"):
            spread(all2, 1 - mc)
            times_green(1 - mc, fourth)

        @pl.when(home)
        def _():
            wait_got(blk.at[pl.ds(0, REP - 1)], 6)
            wait_sent(blk.at[pl.ds(0, REP - 1)], 6)
            blk[eb_own] = fine[...]

        @pl.when(jnp.logical_not(home))
        def _():
            wait_got(blk, 6)
            wait_sent(blk, 6)

        slip_ref[...] = pltpu.roll(blk[...].reshape(NEP, 128), lax.rem(128 - 32 * mr, 128), 1).T
        wait_sent(got.at[pl.ds(1, DEV - 1)], 0)
        wait_sent(brecv.at[pl.ds(1, PEERS - 1)], 1)
        for k in (2, 4, 10, 13):
            wait_sent(recv1.at[pl.ds(1, PEERS - 1)], k)
        wait_sent(bpair, 7)
        for k in (3, 5):
            wait_sent(all1.at[pl.ds(0, 16)], k)
        for k in (8, 9, 11, 12):
            wait_sent(psend1.at[0], k)

    pl.run_scoped(
        solve,
        pltpu.VMEM((NEP, PIX_DEV), F32),
        pltpu.VMEM((2 * NEP, PIX_DEV), BF),
        pltpu.VMEM((NEP, NPATCH // 2), BF),
    )


def on_device(interferograms, epoch_pairs, los, patch_place, patch_depth):
    vm = pl.BlockSpec(memory_space=pltpu.VMEM)
    predicted, slip = pl.pallas_call(
        kernel,
        out_shape=(jax.ShapeDtypeStruct((NEP, PIX_DEV), F32), jax.ShapeDtypeStruct((128, NEP), F32)),
        in_specs=[pl.BlockSpec(memory_space=pltpu.HBM)] * 5,
        out_specs=(vm, vm),
        scratch_shapes=[
            pltpu.VMEM((2, 256), jnp.int32),
            pltpu.VMEM((3, PIX_DEV), F32),
            pltpu.VMEM((2, NPATCH), jnp.int32),
            pltpu.VMEM((1, NPATCH), jnp.int32),
            pltpu.VMEM((DEV, 2, PIX_DEV), BF),
            pltpu.VMEM((NEP, NEP), F32),
            pltpu.VMEM((PIX, 1, 128), F32),
            pltpu.VMEM((DEV, 2, PIX_DEV), BF),
            pltpu.VMEM((16, REP) + CH, BF),
            pltpu.VMEM((16, REP) + CH, BF),
            pltpu.VMEM((PEERS,) + CH, BF),
            pltpu.VMEM((PEERS,) + CH, BF),
            pltpu.VMEM((2, NEP, NCHUNK), BF),
            pltpu.VMEM((2, NEP, NCHUNK), BF),
            pltpu.VMEM((2, NEP, NCHUNK), BF),
            pltpu.VMEM((2, NEP, NCHUNK), BF),
            pltpu.VMEM((16, 1, 128), F32),
            pltpu.VMEM((16, 1, 128), F32),
            pltpu.VMEM((PEERS, 1, 128), F32),
            pltpu.VMEM((2,) + CH, BF),
            pltpu.VMEM((PIX, REP) + CH, BF),
            pltpu.VMEM((PIX, REP) + CH, BF),
            pltpu.VMEM(CH, F32),
            pltpu.VMEM((REP,) + CH, F32),
            pltpu.SemaphoreType.DMA((14,)),
            pltpu.SemaphoreType.DMA((14,)),
            pltpu.SemaphoreType.DMA((5,)),
        ],
        compiler_params=pltpu.CompilerParams(vmem_limit_bytes=60 << 20, has_side_effects=True, collective_id=0),
        name="slip",
    )(interferograms, epoch_pairs, los, patch_place, patch_depth.reshape(1, NPATCH))
    return predicted, slip[:32].T


def solution(mesh):
    placed = (P(("pix", "rep"), None), P(), P(None, ("pix", "rep")), P(), P())
    return jax.shard_map(
        on_device,
        mesh=mesh,
        in_specs=placed,
        out_specs=(P(None, ("pix", "rep")), P(None, ("pix", "rep"))),
        check_vma=False,
    )
```

```python
import functools

import jax
import jax.numpy as jnp
from jax import lax
from jax.experimental import pallas as pl
from jax.experimental.pallas import tpu as pltpu
from jax.sharding import PartitionSpec as P

NEP = 64
NPATCH = 4096
PIX_DEV = 4096
IMG_W = 1024
PIX = 32
REP = 4
DEV = PIX * REP
F32, BF = jnp.float32, jnp.bfloat16
MESH = pl.DeviceIdType.MESH
damping = 0.5


def split(x, n):
    out = []
    for _ in range(n):
        h = x.astype(BF).astype(F32)
        out.append(h)
        x = x - h
    return out

CB, PB = 64, 2048
NCHUNK = 1024
GCHUNK = 2048
PEERS = DEV // 2
CH = (16, 128)


def features(los_ref, place_ref, depth_ref, pixrow, pixcol, patchrow, patchf, prow, srow):
    base = (lax.axis_index("pix") * REP + lax.axis_index("rep")).astype(F32)
    cx = place_ref[0:1, :].astype(F32)
    ny = place_ref[1:2, :].astype(F32)
    d2 = depth_ref[...].astype(F32) + 2.0
    px = cx * 8.0 + 4.0
    py = (ny - base) * 8.0 + 3.0
    h = d2 * 5.0
    prow[0:1, :] = px
    for r in range(4):
        dy = 2.0 * r - py
        srow[r : r + 1, :] = dy * dy + h * h
    f1 = split(d2 * (px - 1024.0), 2)
    f2 = split(d2 * py, 2)
    rows = [d2] * 3 + [-f1[0], -f1[1]] * 3 + [-f2[0], -f2[1]] * 3 + [d2 * h] * 3
    patchrow[...] = jnp.zeros_like(patchrow)
    for k, v in enumerate(rows):
        patchrow[k : k + 1, :] = v
    patchf[...] = patchrow[...].astype(BF)
    g = lax.broadcasted_iota(jnp.int32, (1, PIX_DEV), 1)
    xc = ((g % IMG_W) * 2 + (1 - 1024)).astype(F32)
    yc = ((g // IMG_W) * 2).astype(F32)
    l0 = los_ref[0:1, :] * 100.0
    l1 = los_ref[1:2, :] * 100.0
    l2 = los_ref[2:3, :] * 100.0
    a = split(l0 * xc + l1 * yc, 3)
    s0, s1, s2 = split(l0, 3), split(l1, 3), split(l2, 3)
    rows = a + [s0[0], s0[0], s0[1], s0[1], s0[2], s0[2]] + [s1[0], s1[0], s1[1], s1[1], s1[2], s1[2]] + s2
    pixrow[...] = jnp.zeros_like(pixrow)
    for k, v in enumerate(rows):
        pixrow[k : k + 1, :] = v
    pixcol[...] = pixrow[...].T.astype(BF)


def invert_step(k, a_ref):
    a = a_ref[...]
    kk = lax.rem(k, NEP)
    lane = lax.broadcasted_iota(jnp.int32, (NEP, NEP), 1)
    sub = lax.broadcasted_iota(jnp.int32, (NEP, NEP), 0)
    row = a_ref[pl.ds(kk, 1), :]
    lane1 = lax.broadcasted_iota(jnp.int32, (1, NEP), 1)
    inv = 1.0 / jnp.sum(jnp.where(lane1 == kk, row, 0.0), axis=1, keepdims=True)
    col = jnp.sum(jnp.where(lane == kk, a, 0.0), axis=1, keepdims=True)
    new_row = jnp.where(lane1 == kk, inv, row * inv)
    rest = jnp.where(lane == kk, 0.0, a) - col * new_row
    new = jnp.where(sub == kk, new_row, rest)
    a_ref[...] = jnp.where(k < NEP, new, a)


def for_others(mp, mr, fn):
    for i in range(1, REP):
        fn(mp, lax.rem(mr + i, REP))

    def one(k, _):
        pix = lax.rem(mp + 13 * k, PIX)
        for rep in range(REP):
            fn(pix, rep)
        return 0

    lax.fori_loop(1, PIX, one, 0)


def opening(inputs, places, lsem, xf):
    xb = places[4]
    loads = [pltpu.make_async_copy(src, dst, lsem.at[i]) for i, (src, dst) in enumerate(zip(inputs, (xf,) + tuple(places[:4])))]
    for load in loads:
        load.start()
    ready = pltpu.get_barrier_semaphore()

    def tell(pix, rep):
        pl.semaphore_signal(ready, inc=1, device_id={"pix": pix, "rep": rep}, device_id_type=MESH)

    with jax.named_scope("signal"):
        for_others(lax.axis_index("pix"), lax.axis_index("rep"), tell)
    for load in loads:
        load.wait()

    def one(k, _):
        for u in range(4):
            xb[4 * k + u] = xf[:, pl.ds(pl.multiple_of((4 * k + u) * PIX_DEV, PIX_DEV), PIX_DEV)].astype(BF)
        return 0

    with jax.named_scope("convert"):
        lax.fori_loop(0, DEV // 4, one, 0)


def kernel(*refs):
    pl.run_scoped(functools.partial(opening, refs[:5], refs[7:12], refs[-1]), pltpu.VMEM((2, DEV * PIX_DEV), F32))
    pl.run_scoped(functools.partial(body, *refs), pltpu.VMEM((PIX_DEV, NPATCH), BF))


def body(
    x_hbm, pairs_hbm, los_hbm, place_hbm, depth_hbm, pred_ref, slip_ref,
    pairs_ref, los_ref, place_ref, depth_ref, xb, a_ref, bound_ref,
    got, send1, send2, recv1, recv2, psend1, psend2, precv1, precv2, bpair, bsend, brecv, own, all1, all2, fine, blk,
    ssem, rsem, lsem,
    g_ref,
):
    mp, mr = lax.axis_index("pix"), lax.axis_index("rep")
    me = mp * REP + mr

    def copy(src, dst, k, pix, rep):
        return pltpu.make_async_remote_copy(src, dst, ssem.at[k], rsem.at[k], device_id={"pix": pix, "rep": rep}, device_id_type=MESH)

    def wait_sent(buf, k):
        pltpu.make_async_copy(buf, buf, ssem.at[k]).wait()

    def wait_got(buf, k):
        pltpu.make_async_copy(buf, buf, rsem.at[k]).wait()

    others = functools.partial(for_others, mp, mr)

    mc, mx = lax.rem(mr, 2), mr // 2
    mine_at = 2 * mp + mx
    pb_own, eb_own = 16 * mc + mp // 2, 2 * mx + lax.rem(mp, 2)

    def pair(src, dst, k):
        return copy(src, dst, k, mp, mr + 1 - 2 * mc)

    got_pair = wait_got

    def peers(fn):
        for i in range(1, 4):
            at = lax.rem(2 * lax.rem(mp, 2) + mx + i, 4)
            fn(mp // 2, at // 2, lax.rem(at, 2))

        def one(k, _):
            pp = lax.rem(mp // 2 + 7 * k, 16)
            for half in range(2):
                for xh in range(2):
                    fn(pp, half, xh)
            return 0

        lax.fori_loop(1, 16, one, 0)

    def design():
        epoch = lax.broadcasted_iota(jnp.int32, (NEP, 256), 0)
        return ((epoch == pairs_ref[1:2, :]).astype(F32) - (epoch == pairs_ref[0:1, :]).astype(F32)).astype(BF)

    def build(pixrow, patchrow, prow, srow, wacc, pixcol, patchf, wrow):
        with jax.named_scope("features"):
            features(los_ref, place_ref, depth_ref, pixrow, pixcol, patchrow, patchf, prow, srow)
        with jax.named_scope("wait_ready"):
            pl.semaphore_wait(pltpu.get_barrier_semaphore(), DEV - 1)

        with jax.named_scope("send_ifg"):
            others(lambda pix, rep: copy(xb.at[pix * REP + rep], got.at[me], 0, pix, rep).start())
            got[me] = xb[me]

        with jax.named_scope("normal"):
            design_b = design()
            normal = lax.dot_general(design_b, design_b, (((1,), (1,)), ((), ())), preferred_element_type=F32)
            eye = lax.broadcasted_iota(jnp.int32, (NEP, NEP), 0) == lax.broadcasted_iota(jnp.int32, (NEP, NEP), 1)
            a_ref[...] = normal + jnp.where(eye, damping, 0.0)
            wacc[...] = jnp.zeros_like(wacc)

        def step(it, _):
            invert_step(2 * it, a_ref)
            invert_step(2 * it + 1, a_ref)
            c0 = pl.multiple_of((it // (NPATCH // PB)) * CB, CB)
            p0 = pl.multiple_of(lax.rem(it, NPATCH // PB) * PB, PB)
            xs = (lax.broadcasted_iota(jnp.int32, (CB, 128), 0) * 2 + (2 * c0 + 1)).astype(F32)
            dxs = []
            for q in range(PB // 128):
                dx = xs - prow[0:1, pl.ds(pl.multiple_of(p0 + 128 * q, 128), 128)]
                dxs.append(dx * dx)
            for r in range(4):
                rowsl = pl.ds(pl.multiple_of(r * IMG_W + c0, CB), CB)
                t = jnp.dot(pixcol[rowsl, :], patchf[:, pl.ds(p0, PB)], preferred_element_type=F32)
                acc = wacc[rowsl, :]
                mags = []
                for q in range(PB // 128):
                    ps = pl.ds(pl.multiple_of(p0 + 128 * q, 128), 128)
                    inv = lax.rsqrt(dxs[q] + srow[r : r + 1, ps])
                    gf = (t[:, 128 * q : 128 * q + 128] * (inv * inv * inv)).astype(BF)
                    g_ref[rowsl, ps] = gf
                    mags.append(jnp.abs(gf))
                while len(mags) > PB // 512:
                    mags = [a + b for a, b in zip(mags[0::2], mags[1::2])]
                for m in mags:
                    acc = acc + m.astype(F32)
                wacc[rowsl, :] = acc
            return 0

        with jax.named_scope("green"):
            lax.fori_loop(0, (IMG_W // CB) * (NPATCH // PB), step, 0)

        ones = jnp.ones((16, 128), BF)

        def wstep(j, _):
            sl = pl.ds(pl.multiple_of(j * 2048, 2048), 2048)
            w = jnp.zeros((16, 2048), F32)
            for part in split(wacc[sl, :], 3):
                w = w + lax.dot_general(ones, part.astype(BF), (((1,), (1,)), ((), ())), preferred_element_type=F32)
            wrow[:, sl] = w.astype(BF)
            return 0

        with jax.named_scope("weight"):
            lax.fori_loop(0, 2, wstep, 0)

        def bstep(j, _):
            ps = pl.ds(pl.multiple_of(j * 1024, 1024), 1024)
            b = jnp.dot(wrow[...], jnp.abs(g_ref[:, ps]), preferred_element_type=F32)
            for q in range(8):
                bound_ref[8 * j + q] = b[0:1, 128 * q : 128 * q + 128]
            return 0

        with jax.named_scope("bound"):
            lax.fori_loop(0, 4, bstep, 0)

    pl.run_scoped(
        build,
        pltpu.VMEM((24, PIX_DEV), F32),
        pltpu.VMEM((24, NPATCH), F32),
        pltpu.VMEM((8, NPATCH), F32),
        pltpu.VMEM((8, NPATCH), F32),
        pltpu.VMEM((PIX_DEV, 128), F32),
        pltpu.VMEM((PIX_DEV, 24), BF),
        pltpu.VMEM((24, NPATCH), BF),
        pltpu.VMEM((16, PIX_DEV), BF),
    )

    def solve(series, resid, slipf):
        pair(bound_ref.at[pl.ds(16 * (1 - mc), 16)], bpair, 7).start()

        design_b = design()
        acc = jnp.zeros((NEP, 256), F32)
        for part in split(a_ref[...], 3):
            acc = acc + jnp.dot(part.astype(BF), design_b, preferred_element_type=F32)
        parts = split(acc, 2)
        pseudo = jnp.concatenate(parts, axis=0).astype(BF)
        with jax.named_scope("wait_ifg"):
            wait_got(got.at[pl.ds(1, DEV - 1)], 0)

        def sstep(k, _):
            sl = pl.ds(pl.multiple_of(k * 512, 512), 512)
            out = jnp.dot(pseudo, got[:, :, sl].reshape(256, 512), preferred_element_type=F32)
            ser = out[:NEP] + out[NEP:]
            series[:, sl] = ser
            high, low = split(ser, 2)
            resid[0:NEP, sl] = high.astype(BF)
            resid[NEP : 2 * NEP, sl] = low.astype(BF)
            return 0

        with jax.named_scope("series"):
            lax.fori_loop(0, 8, sstep, 0)

        with jax.named_scope("send_bound"):
            got_pair(bpair, 7)
            bsend[...] = bound_ref[pl.ds(16 * mc, 16)] + bpair[...]
            peers(lambda pp, half, xh: copy(bsend.at[pp], brecv.at[mine_at], 1, 2 * pp + half, 2 * xh + mc).start())
            brecv[mine_at] = bsend[mp // 2]

        def project(send, recv, psend, precv, k):
            def product(pc):
                parts = []
                for q in range(NCHUNK // 512):
                    cols = pl.ds(pl.multiple_of(pc * NCHUNK + 512 * q, 512), 512)
                    out = jnp.dot(resid[...], g_ref[:, cols], preferred_element_type=F32)
                    parts.append(out[:NEP] + out[NEP:])
                return jnp.concatenate(parts, axis=1)

            def push(ch, near):
                for q in range(8):
                    for half in range(2):
                        pix = 2 * (8 * ch + q) + half
                        for xh in range(2):

                            def go():
                                copy(send.at[8 * ch + q, 2 * xh + half], recv.at[mine_at], k + 2, pix, 2 * xh + mc).start()

                            if near:
                                pl.when((pix != mp) | (mx != xh))(go)
                            else:
                                go()

            def keep(ch):
                rhs = product(2 * mc + ch)
                got_pair(precv.at[ch], k + ch)
                rhs = (rhs + precv[ch].astype(F32)).astype(BF)
                for q in range(8):
                    for eb in range(4):
                        send[8 * ch + q, eb] = rhs[16 * eb : 16 * eb + 16, 128 * q : 128 * q + 128]

            with jax.named_scope("give"):
                for j in range(2):
                    psend[j] = product(2 * (1 - mc) + j).astype(BF)
                    pair(psend.at[j], precv.at[j], k + j).start()
            with jax.named_scope("keep"):
                own_ch = mp // 16
                keep(1 - own_ch)
                push(1 - own_ch, False)
                keep(own_ch)
                push(own_ch, True)
            recv[mine_at] = send[mp // 2, eb_own]
            with jax.named_scope("wait_rhs"):
                wait_got(recv.at[pl.ds(1, PEERS - 1)], k + 2)
            return jnp.sum(recv[...].astype(F32), axis=0)

        xl = mp // 16

        def share(buf, i, k_near, k_far):
            def send_to(k, pp, half, xh):
                copy(own.at[i], buf.at[pb_own, eb_own], k, 2 * pp + half, 2 * xh + mc).start()

            def near(n, _):
                pp = 8 * (1 - xl) + lax.rem(mp // 2 + 3 * n, 8)
                for half in range(2):
                    for xh in range(2):
                        send_to(k_near, pp, half, xh)
                return 0

            def far(n, _):
                pp = 8 * xl + lax.rem(mp // 2 + 3 * n, 8)
                for half in range(2):
                    for xh in range(2):
                        send_to(k_far, pp, half, xh)
                return 0

            with jax.named_scope("send_slip"):
                lax.fori_loop(0, 8, near, 0)
                lax.fori_loop(1, 8, far, 0)
                for n in range(1, 4):
                    at = lax.rem(2 * lax.rem(mp, 2) + mx + n, 4)
                    send_to(k_far, mp // 2, at // 2, lax.rem(at, 2))
            buf[pb_own, eb_own] = own[i]

        def times_green(buf, block, count, use):
            for b in range(count):
                slipf[:, 128 * b : 128 * b + 128] = buf[block + b].reshape(NEP, 128)
            cols = pl.ds(pl.multiple_of(block * 128, 1024), 128 * count)

            def one(j, _):
                gs = pl.ds(pl.multiple_of(j * GCHUNK, GCHUNK), GCHUNK)
                part = slipf[:, 0 : 128 * count]
                use(gs, lax.dot_general(part, g_ref[gs, cols], (((1,), (1,)), ((), ())), preferred_element_type=F32))
                return 0

            lax.fori_loop(0, PIX_DEV // GCHUNK, one, 0)

        def all_green(buf, k_near, k_far, k_pair, uses):
            half = pl.ds(16 * mc, 16)
            with jax.named_scope("wait_slip"):
                wait_got(recv1.at[pl.ds(0, 32)], k_near)
            with jax.named_scope("guess"):
                times_green(buf, 16 * mc + 8 * (1 - xl), 8, uses[0])
            with jax.named_scope("wait_far"):
                wait_got(recv1.at[pl.ds(0, 31)], k_far)
            pair(buf.at[half], buf.at[half], k_pair).start()
            with jax.named_scope("guess_far"):
                times_green(buf, 16 * mc + 8 * xl, 8, uses[1])
            got_pair(buf.at[pl.ds(16 * (1 - mc), 16)], k_pair)
            with jax.named_scope("guess2"):
                times_green(buf, 16 * (1 - mc), 16, uses[2])

        rhs = project(send1, recv1, psend1, precv1, 8)
        wait_got(brecv.at[pl.ds(1, PEERS - 1)], 1)
        bound = jnp.sum(brecv[...], axis=0)
        slip = rhs / bound
        own[0] = slip.astype(BF)
        share(all1, 0, 2, 14)

        def first(gs, out):
            series[:, gs] = series[:, gs] - out

        def second(gs, out):
            high, low = split(series[:, gs] - out, 2)
            resid[0:NEP, gs] = high.astype(BF)
            resid[NEP : 2 * NEP, gs] = low.astype(BF)

        all_green(all1, 2, 14, 3, (first, first, second))
        rhs = project(send2, recv2, psend2, precv2, 11)
        slip = slip + rhs / bound
        own[1] = slip.astype(BF)
        fine[...] = slip
        home = pb_own == mp
        for rep in range(REP):

            @pl.when(jnp.logical_not(home) | (mr != rep))
            def _():
                copy(fine, blk.at[eb_own], 6, pb_own, rep).start()

        share(all2, 1, 4, 15)

        def third(gs, out):
            pred_ref[:, gs] = out

        def fourth(gs, out):
            pred_ref[:, gs] = pred_ref[:, gs] + out

        all_green(all2, 4, 15, 5, (third, fourth, fourth))

        @pl.when(home)
        def _():
            wait_got(blk.at[pl.ds(0, REP - 1)], 6)
            wait_sent(blk.at[pl.ds(0, REP - 1)], 6)
            blk[eb_own] = fine[...]

        @pl.when(jnp.logical_not(home))
        def _():
            wait_got(blk, 6)
            wait_sent(blk, 6)

        slip_ref[...] = pltpu.roll(blk[...].reshape(NEP, 128), lax.rem(128 - 32 * mr, 128), 1).T[0:32]
        wait_sent(got.at[pl.ds(1, DEV - 1)], 0)
        wait_sent(brecv.at[pl.ds(1, PEERS - 1)], 1)
        for k in (10, 13):
            wait_sent(recv1.at[pl.ds(1, PEERS - 1)], k)
        for k in (2, 4):
            wait_sent(recv1.at[pl.ds(0, 32)], k)
        for k in (14, 15):
            wait_sent(recv1.at[pl.ds(0, 31)], k)
        wait_sent(bpair, 7)
        for k in (3, 5):
            wait_sent(all1.at[pl.ds(0, 16)], k)
        for k in (8, 9, 11, 12):
            wait_sent(psend1.at[0], k)

    pl.run_scoped(
        solve,
        pltpu.VMEM((NEP, PIX_DEV), F32),
        pltpu.VMEM((2 * NEP, PIX_DEV), BF),
        pltpu.VMEM((NEP, NPATCH // 2), BF),
    )


def on_device(interferograms, epoch_pairs, los, patch_place, patch_depth):
    vm = pl.BlockSpec(memory_space=pltpu.VMEM)
    predicted, slip = pl.pallas_call(
        kernel,
        out_shape=(jax.ShapeDtypeStruct((NEP, PIX_DEV), F32), jax.ShapeDtypeStruct((32, NEP), F32)),
        in_specs=[pl.BlockSpec(memory_space=pltpu.HBM)] * 5,
        out_specs=(vm, vm),
        scratch_shapes=[
            pltpu.VMEM((2, 256), jnp.int32),
            pltpu.VMEM((3, PIX_DEV), F32),
            pltpu.VMEM((2, NPATCH), jnp.int32),
            pltpu.VMEM((1, NPATCH), jnp.int32),
            pltpu.VMEM((DEV, 2, PIX_DEV), BF),
            pltpu.VMEM((NEP, NEP), F32),
            pltpu.VMEM((PIX, 1, 128), F32),
            pltpu.VMEM((DEV, 2, PIX_DEV), BF),
            pltpu.VMEM((16, REP) + CH, BF),
            pltpu.VMEM((16, REP) + CH, BF),
            pltpu.VMEM((PEERS,) + CH, BF),
            pltpu.VMEM((PEERS,) + CH, BF),
            pltpu.VMEM((2, NEP, NCHUNK), BF),
            pltpu.VMEM((2, NEP, NCHUNK), BF),
            pltpu.VMEM((2, NEP, NCHUNK), BF),
            pltpu.VMEM((2, NEP, NCHUNK), BF),
            pltpu.VMEM((16, 1, 128), F32),
            pltpu.VMEM((16, 1, 128), F32),
            pltpu.VMEM((PEERS, 1, 128), F32),
            pltpu.VMEM((2,) + CH, BF),
            pltpu.VMEM((PIX, REP) + CH, BF),
            pltpu.VMEM((PIX, REP) + CH, BF),
            pltpu.VMEM(CH, F32),
            pltpu.VMEM((REP,) + CH, F32),
            pltpu.SemaphoreType.DMA((16,)),
            pltpu.SemaphoreType.DMA((16,)),
            pltpu.SemaphoreType.DMA((5,)),
        ],
        compiler_params=pltpu.CompilerParams(vmem_limit_bytes=60 << 20, has_side_effects=True, collective_id=0),
        name="slip",
    )(interferograms, epoch_pairs, los, patch_place, patch_depth.reshape(1, NPATCH))
    return predicted, slip.T


def solution(mesh):
    placed = (P(("pix", "rep"), None), P(), P(None, ("pix", "rep")), P(), P())
    return jax.shard_map(
        on_device,
        mesh=mesh,
        in_specs=placed,
        out_specs=(P(None, ("pix", "rep")), P(None, ("pix", "rep"))),
        check_vma=False,
    )
```

```python
import functools

import jax
import jax.numpy as jnp
from jax import lax
from jax.experimental import pallas as pl
from jax.experimental.pallas import tpu as pltpu
from jax.sharding import PartitionSpec as P

NEP = 64
NPATCH = 4096
PIX_DEV = 4096
IMG_W = 1024
PIX = 32
REP = 4
DEV = PIX * REP
F32, BF = jnp.float32, jnp.bfloat16
MESH = pl.DeviceIdType.MESH
damping = 0.5


def split(x, n):
    out = []
    for _ in range(n):
        h = x.astype(BF).astype(F32)
        out.append(h)
        x = x - h
    return out

CB, PB = 64, 2048
NCHUNK = 1024
GCHUNK = 2048
PEERS = DEV // 2
CH = (16, 128)


def features(los_ref, place_ref, depth_ref, pixrow, pixcol, patchrow, patchf, prow, srow):
    base = (lax.axis_index("pix") * REP + lax.axis_index("rep")).astype(F32)
    cx = place_ref[0:1, :].astype(F32)
    ny = place_ref[1:2, :].astype(F32)
    d2 = depth_ref[...].astype(F32) + 2.0
    px = cx * 8.0 + 4.0
    py = (ny - base) * 8.0 + 3.0
    h = d2 * 5.0
    prow[0:1, :] = px
    for r in range(4):
        dy = 2.0 * r - py
        srow[r : r + 1, :] = dy * dy + h * h
    f1 = split(d2 * (px - 1024.0), 2)
    f2 = split(d2 * py, 2)
    rows = [d2] * 3 + [-f1[0], -f1[1]] * 3 + [-f2[0], -f2[1]] * 3 + [d2 * h] * 3
    patchrow[...] = jnp.zeros_like(patchrow)
    for k, v in enumerate(rows):
        patchrow[k : k + 1, :] = v
    patchf[...] = patchrow[...].astype(BF)
    g = lax.broadcasted_iota(jnp.int32, (1, PIX_DEV), 1)
    xc = ((g % IMG_W) * 2 + (1 - 1024)).astype(F32)
    yc = ((g // IMG_W) * 2).astype(F32)
    l0 = los_ref[0:1, :] * 100.0
    l1 = los_ref[1:2, :] * 100.0
    l2 = los_ref[2:3, :] * 100.0
    a = split(l0 * xc + l1 * yc, 3)
    s0, s1, s2 = split(l0, 3), split(l1, 3), split(l2, 3)
    rows = a + [s0[0], s0[0], s0[1], s0[1], s0[2], s0[2]] + [s1[0], s1[0], s1[1], s1[1], s1[2], s1[2]] + s2
    pixrow[...] = jnp.zeros_like(pixrow)
    for k, v in enumerate(rows):
        pixrow[k : k + 1, :] = v
    pixcol[...] = pixrow[...].T.astype(BF)


def invert_step(k, a_ref):
    a = a_ref[...]
    kk = lax.rem(k, NEP)
    lane = lax.broadcasted_iota(jnp.int32, (NEP, NEP), 1)
    sub = lax.broadcasted_iota(jnp.int32, (NEP, NEP), 0)
    row = a_ref[pl.ds(kk, 1), :]
    lane1 = lax.broadcasted_iota(jnp.int32, (1, NEP), 1)
    inv = 1.0 / jnp.sum(jnp.where(lane1 == kk, row, 0.0), axis=1, keepdims=True)
    col = jnp.sum(jnp.where(lane == kk, a, 0.0), axis=1, keepdims=True)
    new_row = jnp.where(lane1 == kk, inv, row * inv)
    rest = jnp.where(lane == kk, 0.0, a) - col * new_row
    new = jnp.where(sub == kk, new_row, rest)
    a_ref[...] = jnp.where(k < NEP, new, a)


def for_others(mp, mr, fn):
    for i in range(1, REP):
        fn(mp, lax.rem(mr + i, REP))

    def one(k, _):
        pix = lax.rem(mp + 13 * k, PIX)
        for rep in range(REP):
            fn(pix, rep)
        return 0

    lax.fori_loop(1, PIX, one, 0)


def opening(inputs, places, lsem, xf):
    xb = places[4]
    loads = [pltpu.make_async_copy(src, dst, lsem.at[i]) for i, (src, dst) in enumerate(zip(inputs, (xf,) + tuple(places[:4])))]
    for load in loads:
        load.start()
    ready = pltpu.get_barrier_semaphore()

    def tell(pix, rep):
        pl.semaphore_signal(ready, inc=1, device_id={"pix": pix, "rep": rep}, device_id_type=MESH)

    with jax.named_scope("signal"):
        for_others(lax.axis_index("pix"), lax.axis_index("rep"), tell)
    for load in loads:
        load.wait()

    def one(k, _):
        for u in range(4):
            xb[4 * k + u] = xf[:, pl.ds(pl.multiple_of((4 * k + u) * PIX_DEV, PIX_DEV), PIX_DEV)].astype(BF)
        return 0

    with jax.named_scope("convert"):
        lax.fori_loop(0, DEV // 4, one, 0)


def kernel(*refs):
    pl.run_scoped(functools.partial(opening, refs[:5], refs[7:12], refs[-1]), pltpu.VMEM((2, DEV * PIX_DEV), F32))
    pl.run_scoped(functools.partial(body, *refs), pltpu.VMEM((PIX_DEV, NPATCH), BF))


def body(
    x_hbm, pairs_hbm, los_hbm, place_hbm, depth_hbm, pred_ref, slip_ref,
    pairs_ref, los_ref, place_ref, depth_ref, xb, a_ref, bound_ref,
    got, send1, send2, recv1, recv2, psend1, psend2, precv1, precv2, bpair, bsend, brecv, own, all1, all2, fine, blk,
    ssem, rsem, lsem,
    g_ref,
):
    mp, mr = lax.axis_index("pix"), lax.axis_index("rep")
    me = mp * REP + mr

    def copy(src, dst, k, pix, rep):
        return pltpu.make_async_remote_copy(src, dst, ssem.at[k], rsem.at[k], device_id={"pix": pix, "rep": rep}, device_id_type=MESH)

    def wait_sent(buf, k):
        pltpu.make_async_copy(buf, buf, ssem.at[k]).wait()

    def wait_got(buf, k):
        pltpu.make_async_copy(buf, buf, rsem.at[k]).wait()

    others = functools.partial(for_others, mp, mr)

    mc, mx = lax.rem(mr, 2), mr // 2
    mine_at = 2 * mp + mx
    pb_own, eb_own = 16 * mc + mp // 2, 2 * mx + lax.rem(mp, 2)

    def pair(src, dst, k):
        return copy(src, dst, k, mp, mr + 1 - 2 * mc)

    got_pair = wait_got

    def peers(fn):
        for i in range(1, 4):
            at = lax.rem(2 * lax.rem(mp, 2) + mx + i, 4)
            fn(mp // 2, at // 2, lax.rem(at, 2))

        def one(k, _):
            pp = lax.rem(mp // 2 + 7 * k, 16)
            for half in range(2):
                for xh in range(2):
                    fn(pp, half, xh)
            return 0

        for k in range(1, 16):
            one(k, 0)

    def design():
        epoch = lax.broadcasted_iota(jnp.int32, (NEP, 256), 0)
        return ((epoch == pairs_ref[1:2, :]).astype(F32) - (epoch == pairs_ref[0:1, :]).astype(F32)).astype(BF)

    def build(pixrow, patchrow, prow, srow, wacc, pixcol, patchf, wrow):
        with jax.named_scope("features"):
            features(los_ref, place_ref, depth_ref, pixrow, pixcol, patchrow, patchf, prow, srow)
        with jax.named_scope("wait_ready"):
            pl.semaphore_wait(pltpu.get_barrier_semaphore(), DEV - 1)

        with jax.named_scope("send_ifg"):
            others(lambda pix, rep: copy(xb.at[pix * REP + rep], got.at[me], 0, pix, rep).start())
            got[me] = xb[me]

        with jax.named_scope("normal"):
            design_b = design()
            normal = lax.dot_general(design_b, design_b, (((1,), (1,)), ((), ())), preferred_element_type=F32)
            eye = lax.broadcasted_iota(jnp.int32, (NEP, NEP), 0) == lax.broadcasted_iota(jnp.int32, (NEP, NEP), 1)
            a_ref[...] = normal + jnp.where(eye, damping, 0.0)
            wacc[...] = jnp.zeros_like(wacc)

        def step(it, _):
            invert_step(2 * it, a_ref)
            invert_step(2 * it + 1, a_ref)
            c0 = pl.multiple_of((it // (NPATCH // PB)) * CB, CB)
            p0 = pl.multiple_of(lax.rem(it, NPATCH // PB) * PB, PB)
            xs = (lax.broadcasted_iota(jnp.int32, (CB, 128), 0) * 2 + (2 * c0 + 1)).astype(F32)
            dxs = []
            for q in range(PB // 128):
                dx = xs - prow[0:1, pl.ds(pl.multiple_of(p0 + 128 * q, 128), 128)]
                dxs.append(dx * dx)
            for r in range(4):
                rowsl = pl.ds(pl.multiple_of(r * IMG_W + c0, CB), CB)
                t = jnp.dot(pixcol[rowsl, :], patchf[:, pl.ds(p0, PB)], preferred_element_type=F32)
                acc = wacc[rowsl, :]
                mags = []
                for q in range(PB // 128):
                    ps = pl.ds(pl.multiple_of(p0 + 128 * q, 128), 128)
                    inv = lax.rsqrt(dxs[q] + srow[r : r + 1, ps])
                    gf = (t[:, 128 * q : 128 * q + 128] * (inv * inv * inv)).astype(BF)
                    g_ref[rowsl, ps] = gf
                    mags.append(jnp.abs(gf))
                while len(mags) > PB // 512:
                    mags = [a + b for a, b in zip(mags[0::2], mags[1::2])]
                for m in mags:
                    acc = acc + m.astype(F32)
                wacc[rowsl, :] = acc
            return 0

        with jax.named_scope("green"):
            lax.fori_loop(0, (IMG_W // CB) * (NPATCH // PB), step, 0)

        ones = jnp.ones((16, 128), BF)

        def wstep(j, _):
            sl = pl.ds(pl.multiple_of(j * 2048, 2048), 2048)
            w = jnp.zeros((16, 2048), F32)
            for part in split(wacc[sl, :], 3):
                w = w + lax.dot_general(ones, part.astype(BF), (((1,), (1,)), ((), ())), preferred_element_type=F32)
            wrow[:, sl] = w.astype(BF)
            return 0

        with jax.named_scope("weight"):
            lax.fori_loop(0, 2, wstep, 0)

        def bstep(j, _):
            ps = pl.ds(pl.multiple_of(j * 1024, 1024), 1024)
            b = jnp.dot(wrow[...], jnp.abs(g_ref[:, ps]), preferred_element_type=F32)
            for q in range(8):
                bound_ref[8 * j + q] = b[0:1, 128 * q : 128 * q + 128]
            return 0

        with jax.named_scope("bound"):
            lax.fori_loop(0, 4, bstep, 0)

    pl.run_scoped(
        build,
        pltpu.VMEM((24, PIX_DEV), F32),
        pltpu.VMEM((24, NPATCH), F32),
        pltpu.VMEM((8, NPATCH), F32),
        pltpu.VMEM((8, NPATCH), F32),
        pltpu.VMEM((PIX_DEV, 128), F32),
        pltpu.VMEM((PIX_DEV, 24), BF),
        pltpu.VMEM((24, NPATCH), BF),
        pltpu.VMEM((16, PIX_DEV), BF),
    )

    def solve(series, resid, slipf):
        pair(bound_ref.at[pl.ds(16 * (1 - mc), 16)], bpair, 7).start()

        design_b = design()
        acc = jnp.zeros((NEP, 256), F32)
        for part in split(a_ref[...], 3):
            acc = acc + jnp.dot(part.astype(BF), design_b, preferred_element_type=F32)
        parts = split(acc, 2)
        pseudo = jnp.concatenate(parts, axis=0).astype(BF)
        with jax.named_scope("wait_ifg"):
            wait_got(got.at[pl.ds(1, DEV - 1)], 0)

        def sstep(k, _):
            sl = pl.ds(pl.multiple_of(k * 512, 512), 512)
            out = jnp.dot(pseudo, got[:, :, sl].reshape(256, 512), preferred_element_type=F32)
            ser = out[:NEP] + out[NEP:]
            series[:, sl] = ser
            high, low = split(ser, 2)
            resid[0:NEP, sl] = high.astype(BF)
            resid[NEP : 2 * NEP, sl] = low.astype(BF)
            return 0

        with jax.named_scope("series"):
            lax.fori_loop(0, 8, sstep, 0)

        with jax.named_scope("send_bound"):
            got_pair(bpair, 7)
            bsend[...] = bound_ref[pl.ds(16 * mc, 16)] + bpair[...]
            peers(lambda pp, half, xh: copy(bsend.at[pp], brecv.at[mine_at], 1, 2 * pp + half, 2 * xh + mc).start())
            brecv[mine_at] = bsend[mp // 2]

        def project(send, recv, psend, precv, k):
            def product(pc):
                parts = []
                for q in range(NCHUNK // 512):
                    cols = pl.ds(pl.multiple_of(pc * NCHUNK + 512 * q, 512), 512)
                    out = jnp.dot(resid[...], g_ref[:, cols], preferred_element_type=F32)
                    parts.append(out[:NEP] + out[NEP:])
                return jnp.concatenate(parts, axis=1)

            def push(ch, near):
                for q in range(8):
                    for half in range(2):
                        pix = 2 * (8 * ch + q) + half
                        for xh in range(2):

                            def go():
                                copy(send.at[8 * ch + q, 2 * xh + half], recv.at[mine_at], k + 2, pix, 2 * xh + mc).start()

                            if near:
                                pl.when((pix != mp) | (mx != xh))(go)
                            else:
                                go()

            def keep(ch):
                rhs = product(2 * mc + ch)
                got_pair(precv.at[ch], k + ch)
                rhs = (rhs + precv[ch].astype(F32)).astype(BF)
                for q in range(8):
                    for eb in range(4):
                        send[8 * ch + q, eb] = rhs[16 * eb : 16 * eb + 16, 128 * q : 128 * q + 128]

            with jax.named_scope("give"):
                for j in range(2):
                    psend[j] = product(2 * (1 - mc) + j).astype(BF)
                    pair(psend.at[j], precv.at[j], k + j).start()
            with jax.named_scope("keep"):
                own_ch = mp // 16
                keep(1 - own_ch)
                push(1 - own_ch, False)
                keep(own_ch)
                push(own_ch, True)
            recv[mine_at] = send[mp // 2, eb_own]
            with jax.named_scope("wait_rhs"):
                wait_got(recv.at[pl.ds(1, PEERS - 1)], k + 2)
            return jnp.sum(recv[...].astype(F32), axis=0)

        xl = mp // 16

        def share(buf, i, k_near, k_far):
            def send_to(k, pp, half, xh):
                copy(own.at[i], buf.at[pb_own, eb_own], k, 2 * pp + half, 2 * xh + mc).start()

            def near(n, _):
                pp = 8 * (1 - xl) + lax.rem(mp // 2 + 3 * n, 8)
                for half in range(2):
                    for xh in range(2):
                        send_to(k_near, pp, half, xh)
                return 0

            def far(n, _):
                pp = 8 * xl + lax.rem(mp // 2 + 3 * n, 8)
                for half in range(2):
                    for xh in range(2):
                        send_to(k_far, pp, half, xh)
                return 0

            with jax.named_scope("send_slip"):
                lax.fori_loop(0, 8, near, 0)
                lax.fori_loop(1, 8, far, 0)
                for n in range(1, 4):
                    at = lax.rem(2 * lax.rem(mp, 2) + mx + n, 4)
                    send_to(k_far, mp // 2, at // 2, lax.rem(at, 2))
            buf[pb_own, eb_own] = own[i]

        def times_green(buf, block, count, use):
            for b in range(count):
                slipf[:, 128 * b : 128 * b + 128] = buf[block + b].reshape(NEP, 128)
            cols = pl.ds(pl.multiple_of(block * 128, 1024), 128 * count)

            def one(j, _):
                gs = pl.ds(pl.multiple_of(j * GCHUNK, GCHUNK), GCHUNK)
                part = slipf[:, 0 : 128 * count]
                use(gs, lax.dot_general(part, g_ref[gs, cols], (((1,), (1,)), ((), ())), preferred_element_type=F32))
                return 0

            lax.fori_loop(0, PIX_DEV // GCHUNK, one, 0)

        def all_green(buf, k_near, k_far, k_pair, uses):
            half = pl.ds(16 * mc, 16)
            with jax.named_scope("wait_slip"):
                wait_got(recv1.at[pl.ds(0, 32)], k_near)
            with jax.named_scope("guess"):
                times_green(buf, 16 * mc + 8 * (1 - xl), 8, uses[0])
            with jax.named_scope("wait_far"):
                wait_got(recv1.at[pl.ds(0, 31)], k_far)
            pair(buf.at[half], buf.at[half], k_pair).start()
            with jax.named_scope("guess_far"):
                times_green(buf, 16 * mc + 8 * xl, 8, uses[1])
            got_pair(buf.at[pl.ds(16 * (1 - mc), 16)], k_pair)
            with jax.named_scope("guess2"):
                times_green(buf, 16 * (1 - mc), 16, uses[2])

        rhs = project(send1, recv1, psend1, precv1, 8)
        wait_got(brecv.at[pl.ds(1, PEERS - 1)], 1)
        bound = jnp.sum(brecv[...], axis=0)
        slip = rhs / bound
        own[0] = slip.astype(BF)
        share(all1, 0, 2, 14)

        def first(gs, out):
            series[:, gs] = series[:, gs] - out

        def second(gs, out):
            high, low = split(series[:, gs] - out, 2)
            resid[0:NEP, gs] = high.astype(BF)
            resid[NEP : 2 * NEP, gs] = low.astype(BF)

        all_green(all1, 2, 14, 3, (first, first, second))
        rhs = project(send2, recv2, psend2, precv2, 11)
        slip = slip + rhs / bound
        own[1] = slip.astype(BF)
        fine[...] = slip
        home = pb_own == mp
        for rep in range(REP):

            @pl.when(jnp.logical_not(home) | (mr != rep))
            def _():
                copy(fine, blk.at[eb_own], 6, pb_own, rep).start()

        share(all2, 1, 4, 15)

        def third(gs, out):
            pred_ref[:, gs] = out

        def fourth(gs, out):
            pred_ref[:, gs] = pred_ref[:, gs] + out

        all_green(all2, 4, 15, 5, (third, fourth, fourth))

        @pl.when(home)
        def _():
            wait_got(blk.at[pl.ds(0, REP - 1)], 6)
            wait_sent(blk.at[pl.ds(0, REP - 1)], 6)
            blk[eb_own] = fine[...]

        @pl.when(jnp.logical_not(home))
        def _():
            wait_got(blk, 6)
            wait_sent(blk, 6)

        slip_ref[...] = pltpu.roll(blk[...].reshape(NEP, 128), lax.rem(128 - 32 * mr, 128), 1).T[0:32]
        wait_sent(got.at[pl.ds(1, DEV - 1)], 0)
        wait_sent(brecv.at[pl.ds(1, PEERS - 1)], 1)
        for k in (10, 13):
            wait_sent(recv1.at[pl.ds(1, PEERS - 1)], k)
        for k in (2, 4):
            wait_sent(recv1.at[pl.ds(0, 32)], k)
        for k in (14, 15):
            wait_sent(recv1.at[pl.ds(0, 31)], k)
        wait_sent(bpair, 7)
        for k in (3, 5):
            wait_sent(all1.at[pl.ds(0, 16)], k)
        for k in (8, 9, 11, 12):
            wait_sent(psend1.at[0], k)

    pl.run_scoped(
        solve,
        pltpu.VMEM((NEP, PIX_DEV), F32),
        pltpu.VMEM((2 * NEP, PIX_DEV), BF),
        pltpu.VMEM((NEP, NPATCH // 2), BF),
    )


def on_device(interferograms, epoch_pairs, los, patch_place, patch_depth):
    vm = pl.BlockSpec(memory_space=pltpu.VMEM)
    predicted, slip = pl.pallas_call(
        kernel,
        out_shape=(jax.ShapeDtypeStruct((NEP, PIX_DEV), F32), jax.ShapeDtypeStruct((32, NEP), F32)),
        in_specs=[pl.BlockSpec(memory_space=pltpu.HBM)] * 5,
        out_specs=(vm, vm),
        scratch_shapes=[
            pltpu.VMEM((2, 256), jnp.int32),
            pltpu.VMEM((3, PIX_DEV), F32),
            pltpu.VMEM((2, NPATCH), jnp.int32),
            pltpu.VMEM((1, NPATCH), jnp.int32),
            pltpu.VMEM((DEV, 2, PIX_DEV), BF),
            pltpu.VMEM((NEP, NEP), F32),
            pltpu.VMEM((PIX, 1, 128), F32),
            pltpu.VMEM((DEV, 2, PIX_DEV), BF),
            pltpu.VMEM((16, REP) + CH, BF),
            pltpu.VMEM((16, REP) + CH, BF),
            pltpu.VMEM((PEERS,) + CH, BF),
            pltpu.VMEM((PEERS,) + CH, BF),
            pltpu.VMEM((2, NEP, NCHUNK), BF),
            pltpu.VMEM((2, NEP, NCHUNK), BF),
            pltpu.VMEM((2, NEP, NCHUNK), BF),
            pltpu.VMEM((2, NEP, NCHUNK), BF),
            pltpu.VMEM((16, 1, 128), F32),
            pltpu.VMEM((16, 1, 128), F32),
            pltpu.VMEM((PEERS, 1, 128), F32),
            pltpu.VMEM((2,) + CH, BF),
            pltpu.VMEM((PIX, REP) + CH, BF),
            pltpu.VMEM((PIX, REP) + CH, BF),
            pltpu.VMEM(CH, F32),
            pltpu.VMEM((REP,) + CH, F32),
            pltpu.SemaphoreType.DMA((16,)),
            pltpu.SemaphoreType.DMA((16,)),
            pltpu.SemaphoreType.DMA((5,)),
        ],
        compiler_params=pltpu.CompilerParams(vmem_limit_bytes=60 << 20, has_side_effects=True, collective_id=0),
        name="slip",
    )(interferograms, epoch_pairs, los, patch_place, patch_depth.reshape(1, NPATCH))
    return predicted, slip.T


def solution(mesh):
    placed = (P(("pix", "rep"), None), P(), P(None, ("pix", "rep")), P(), P())
    return jax.shard_map(
        on_device,
        mesh=mesh,
        in_specs=placed,
        out_specs=(P(None, ("pix", "rep")), P(None, ("pix", "rep"))),
        check_vma=False,
    )
```
